32 devices in a mesh: dp: 1 (over z), ep: 32 (over y, x, core).
Axes of the slice: x: 4, y: 4, z: 1, core: 2. Of those that a mesh axis runs over, the one named last changes fastest.
The devices are a block of a 4x4x8 slice.
Arguments:
- tokens: bfloat16 [32, 1024, 768], P(('dp', 'ep'))
- w_gate: bfloat16 [768, 64], replicated
- expert_ids: int32 [32, 1024, 2], P(('dp', 'ep'))
- keep_second: int32 [32, 1024], P(('dp', 'ep'))
- w_in: bfloat16 [64, 768, 3072], P('ep')
- w_out: bfloat16 [64, 3072, 768], P('ep')
Outputs:
- output: bfloat16 [32, 1024, 768], P(('dp', 'ep'))
All inputs are finite; a program needn't handle non-finite values.
Results may differ from the reference program's by a relative error of at most 0.001.
Values are sent between devices in bfloat16 or wider.
A program may use at most 768 MiB of HBM per device.

```python
import functools
import jax
import jax.numpy as jnp
from jax import lax

GROUPS = 32
TOKENS = 1024
MODEL_DIM = 768
HIDDEN = 3072
EXPERTS = 64
CAPACITY = 2 * TOKENS // EXPERTS


def draw_routing(route_key):
    k_cover, k_raw, k_shift, k_second, k_keep = jax.random.split(route_key, 5)
    cover_keys = jax.random.split(k_cover, GROUPS)
    cover_ids = jax.vmap(functools.partial(jax.random.permutation, x=EXPERTS))(cover_keys)
    hot_shift = jax.random.randint(k_shift, (), 0, EXPERTS)
    raw_ids = jax.random.randint(k_raw, (GROUPS, TOKENS - EXPERTS), 0, EXPERTS + EXPERTS // 2)
    rest_ids = (raw_ids % EXPERTS + hot_shift) % EXPERTS
    first_ids = jnp.concatenate([cover_ids.astype(jnp.int32), rest_ids.astype(jnp.int32)], axis=1)
    second_ids = (first_ids + jax.random.randint(k_second, (GROUPS, TOKENS), 1, EXPERTS)) % EXPERTS
    keep_second = (jax.random.randint(k_keep, (GROUPS, TOKENS), 0, 10) < 9).astype(jnp.int32)
    expert_ids = jnp.stack([first_ids, second_ids], axis=-1).astype(jnp.int32)
    return expert_ids, keep_second


def setup_inputs(seed: int = 0, part: int = 0) -> dict:
    shared_key, parts_key = jax.random.split(jax.random.key(seed))
    part_key = jax.random.fold_in(parts_key, part)
    k_tokens, k_route = jax.random.split(part_key)
    k_gate, k_in, k_out = jax.random.split(shared_key, 3)
    tokens = jax.random.normal(k_tokens, (GROUPS, TOKENS, MODEL_DIM), jnp.float32).astype(jnp.bfloat16)
    expert_ids, keep_second = draw_routing(k_route)
    w_gate = (jax.random.normal(k_gate, (MODEL_DIM, EXPERTS), jnp.float32) * MODEL_DIM ** -0.5).astype(jnp.bfloat16)
    w_in = (jax.random.normal(k_in, (EXPERTS, MODEL_DIM, HIDDEN), jnp.float32) * MODEL_DIM ** -0.5).astype(jnp.bfloat16)
    w_out = (jax.random.normal(k_out, (EXPERTS, HIDDEN, MODEL_DIM), jnp.float32) * (2.0 / HIDDEN) ** 0.5).astype(jnp.bfloat16)
    return {"tokens": tokens, "w_gate": w_gate, "expert_ids": expert_ids, "keep_second": keep_second, "w_in": w_in, "w_out": w_out}


def group_routing(group_tok, group_ids, group_keep, w_gate):
    logits = jnp.dot(group_tok, w_gate, preferred_element_type=jnp.float32)
    gate_probs = jax.nn.softmax(logits, axis=-1)
    first_hot = jax.nn.one_hot(group_ids[:, 0], EXPERTS, dtype=jnp.int32)
    second_hot = jax.nn.one_hot(group_ids[:, 1], EXPERTS, dtype=jnp.int32) * group_keep[:, None]
    gate_first = jnp.sum(gate_probs * first_hot, axis=-1)
    gate_second = jnp.sum(gate_probs * second_hot, axis=-1)
    gate_total = gate_first + gate_second
    gate_first = gate_first / gate_total
    gate_second = gate_second / gate_total
    pos_first = jnp.sum((jnp.cumsum(first_hot, axis=0) - first_hot) * first_hot, axis=-1)
    second_base = jnp.cumsum(second_hot, axis=0) - second_hot + jnp.sum(first_hot, axis=0)[None, :]
    pos_second = jnp.sum(second_base * second_hot, axis=-1)
    slot_first = first_hot[:, :, None] * jax.nn.one_hot(pos_first, CAPACITY, dtype=jnp.float32)[:, None, :]
    slot_second = second_hot[:, :, None] * jax.nn.one_hot(pos_second, CAPACITY, dtype=jnp.float32)[:, None, :]
    dispatch = slot_first + slot_second
    combine = (gate_first[:, None, None] * slot_first + gate_second[:, None, None] * slot_second).astype(jnp.bfloat16)
    return dispatch, combine


def reference(tokens, w_gate, expert_ids, keep_second, w_in, w_out):
    def dispatch_group(operands):
        group_tok, group_ids, group_keep = operands
        dispatch, _ = group_routing(group_tok, group_ids, group_keep, w_gate)
        sent_rows = jnp.einsum("sec,sm->ecm", dispatch.astype(jnp.float32), group_tok.astype(jnp.float32))
        return sent_rows.astype(jnp.bfloat16)

    expert_in = lax.map(dispatch_group, (tokens, expert_ids, keep_second))
    expert_in = jnp.transpose(expert_in, (1, 0, 2, 3))

    def expert_ffn(operands):
        rows_in, w_first, w_second = operands
        flat_rows = rows_in.reshape(GROUPS * CAPACITY, MODEL_DIM)
        hidden = jax.nn.relu(jnp.dot(flat_rows, w_first, preferred_element_type=jnp.float32)).astype(jnp.bfloat16)
        rows_out = jnp.dot(hidden, w_second, preferred_element_type=jnp.float32).astype(jnp.bfloat16)
        return rows_out.reshape(GROUPS, CAPACITY, MODEL_DIM)

    expert_out = lax.map(expert_ffn, (expert_in, w_in, w_out))
    expert_out = jnp.transpose(expert_out, (1, 0, 2, 3))

    def combine_group(operands):
        group_tok, group_ids, group_keep, rows_back = operands
        _, combine = group_routing(group_tok, group_ids, group_keep, w_gate)
        mixed_rows = jnp.einsum("sec,ecm->sm", combine.astype(jnp.float32), rows_back.astype(jnp.float32))
        return mixed_rows.astype(jnp.bfloat16)

    return lax.map(combine_group, (tokens, expert_ids, keep_second, expert_out))
```

```python
import functools
import math

import jax
import jax.numpy as jnp
from jax import lax
from jax.experimental import pallas as pl
from jax.experimental.pallas import tpu as pltpu
from jax.sharding import PartitionSpec as P

F32 = jnp.float32
BF16 = jnp.bfloat16
MESH = pl.DeviceIdType.MESH
CHUNK = 8


def step_offsets(side):
    hop = lambda d: min(d, side - d)
    chips = [(dy, dx) for dy in range(side) for dx in range(side)]
    kinds = [(2, 1), (1, 1), (2, 2), (2, 0), (0, 0), (1, 0)]
    order = []
    for kind in kinds:
        same = [c for c in chips if tuple(sorted((hop(c[0]), hop(c[1])), reverse=True)) == kind]
        order += [(dy, dx, core) for core in range(2) for (dy, dx) in same]
    return order


def layer_kernel(
    n, offsets, tok_hbm, wg_hbm, ids_hbm, keep_hbm, wi_hbm, wo_hbm, out_ref,
    tok, wg, ids, keep, wi, wo, onehot, send, recv, back, home, cols, cw, acc,
    local_sem, fs_sem, fr_sem, bs_sem, br_sem,
):
    side = math.isqrt(n // 2)
    token_count, model_dim = tok.shape
    expert_count = wg.shape[0]
    local_experts, _, hidden_dim = wi.shape
    steps, rows, _ = send.shape
    capacity = rows // local_experts
    chunks = steps // CHUNK
    span = CHUNK * rows
    self_step = offsets.index((0, 0, 0))

    loads = [
        pltpu.make_async_copy(src, dst, local_sem.at[i])
        for i, (src, dst) in enumerate([(ids_hbm, ids), (keep_hbm, keep), (tok_hbm, tok), (wg_hbm, wg)])
    ]
    for e in range(local_experts):
        loads.append(pltpu.make_async_copy(wi_hbm.at[e], wi.at[e], local_sem.at[4 + 2 * e]))
        loads.append(pltpu.make_async_copy(wo_hbm.at[e], wo.at[e], local_sem.at[5 + 2 * e]))
    for load in loads[:4]:
        load.start()

    barrier = pltpu.get_barrier_semaphore()

    @pl.loop(0, n)
    def _(k):
        pl.semaphore_signal(barrier, inc=1, device_id={"ep": k}, device_id_type=MESH)

    me = lax.axis_index("ep")
    my_y, my_x, my_core = me // (2 * side), (me // 2) % side, me % 2

    def peer(step, sign):
        dy, dx, core = offsets[step]
        y, x = (my_y + sign * dy + side) % side, (my_x + sign * dx + side) % side
        return (y * side + x) * 2 + (my_core + core) % 2

    dst = [peer(k, 1) for k in range(steps)]
    src = [peer(k, -1) for k in range(steps)]

    def remote(buf_from, buf_to, ssem, rsem, k, device):
        return pltpu.make_async_remote_copy(
            src_ref=buf_from.at[k], dst_ref=buf_to.at[k], send_sem=ssem.at[k], recv_sem=rsem.at[k],
            device_id={"ep": device}, device_id_type=MESH)

    forth = [remote(send, recv, fs_sem, fr_sem, k, dst[k]) for k in range(steps)]
    home_copy = [remote(back, home, bs_sem, br_sem, k, src[k]) for k in range(steps)]

    loads[0].wait()
    loads[1].wait()
    first_id, second_id = ids[0:1, :], ids[1:2, :]
    used = keep[...] == 1
    expert_row = lax.broadcasted_iota(jnp.int32, (expert_count, token_count), 0)
    first_hot = jnp.where(expert_row == first_id, 1.0, 0.0).astype(F32)
    second_hot = jnp.where((expert_row == second_id) & used, 1.0, 0.0).astype(F32)
    first_total = jnp.sum(first_hot, axis=1, keepdims=True)
    both = jnp.concatenate([first_hot, second_hot], axis=0)
    both16 = both.astype(BF16)
    width = 256
    before = jnp.where(
        lax.broadcasted_iota(jnp.int32, (width, width), 0) < lax.broadcasted_iota(jnp.int32, (width, width), 1),
        1.0, 0.0).astype(BF16)
    carry = jnp.concatenate([jnp.zeros((expert_count, 1), F32), first_total], axis=0)
    pos = []
    for b in range(token_count // width):
        part = both[:, b * width:(b + 1) * width]
        ahead = jnp.dot(both16[:, b * width:(b + 1) * width], before, preferred_element_type=F32) + carry
        picked = part * ahead
        pos.append((jnp.sum(picked[:expert_count], axis=0, keepdims=True), jnp.sum(picked[expert_count:], axis=0, keepdims=True)))
        carry = carry + jnp.sum(part, axis=1, keepdims=True)
    pos_first = jnp.concatenate([p[0] for p in pos], axis=1).astype(jnp.int32)
    pos_second = jnp.concatenate([p[1] for p in pos], axis=1).astype(jnp.int32)
    slot_first = jnp.where(pos_first < capacity, first_id * capacity + pos_first, -1)
    slot_second = jnp.where(used & (pos_second < capacity), second_id * capacity + pos_second, -1)

    loads[2].wait()
    for c in range(chunks):
        for j in range(CHUNK):
            slot = dst[c * CHUNK + j] * rows + lax.broadcasted_iota(jnp.int32, (rows, token_count), 0)
            hit = (slot == slot_first) | (slot == slot_second)
            onehot[j * rows:(j + 1) * rows, :] = jnp.where(hit, 1.0, 0.0).astype(BF16)
        for col in range(0, model_dim, width):
            picked = jnp.dot(onehot[...], tok[:, col:col + width], preferred_element_type=F32).astype(BF16)
            for j in range(CHUNK):
                k = c * CHUNK + j
                target = recv if k == self_step else send
                target[k, :, col:col + width] = picked[j * rows:(j + 1) * rows]
        if c == 0:
            pl.semaphore_wait(barrier, n)
        for k in range(c * CHUNK, (c + 1) * CHUNK):
            if k != self_step:
                forth[k].start()
        if c == 0:
            for load in loads[4:]:
                load.start()

    loads[3].wait()
    logits = lax.dot_general(wg[...], tok[...], (((1,), (1,)), ((), ())), preferred_element_type=F32)
    top = jnp.max(logits, axis=0, keepdims=True)
    raised = jnp.exp(logits - top)
    probs = raised / jnp.sum(raised, axis=0, keepdims=True)
    expert_row = lax.broadcasted_iota(jnp.int32, (expert_count, token_count), 0)
    gate_first = jnp.sum(jnp.where(expert_row == first_id, probs, 0.0), axis=0, keepdims=True)
    gate_second = jnp.sum(jnp.where((expert_row == second_id) & used, probs, 0.0), axis=0, keepdims=True)
    gate_total = gate_first + gate_second
    lines = jnp.concatenate(
        [slot_first.astype(F32), slot_second.astype(F32), gate_first / gate_total, gate_second / gate_total,
         jnp.zeros((124, token_count), F32)], axis=0)
    cols[...] = jnp.transpose(lines)
    block = 64
    for c in range(chunks):
        lane = lax.broadcasted_iota(jnp.int32, (1, span), 1)
        slot = lane % rows
        for j in range(CHUNK):
            slot = slot + jnp.where(lane // rows == j, dst[c * CHUNK + j] * rows, 0)
        slot = slot.astype(F32)

        @pl.loop(0, token_count // block)
        def _(i):
            r = pl.ds(pl.multiple_of(i * block, block), block)
            line = cols[r, :]
            weight = jnp.where(line[:, 0:1] == slot, line[:, 2:3], 0.0) + jnp.where(line[:, 1:2] == slot, line[:, 3:4], 0.0)
            cw[r, c * span:(c + 1) * span] = weight.astype(BF16)

    for load in loads[4:]:
        load.wait()
    for c in range(chunks):
        for k in range(c * CHUNK, (c + 1) * CHUNK):
            if k != self_step:
                forth[k].wait_recv()

        @pl.loop(0, local_experts)
        def _(e):
            r = pl.ds(pl.multiple_of(e * capacity, capacity), capacity)
            x = recv[c * CHUNK:(c + 1) * CHUNK, r, :].reshape(CHUNK * capacity, model_dim)
            y = jnp.zeros((CHUNK * capacity, model_dim), F32)
            tile = 768
            for h in range(0, hidden_dim, tile):
                hidden = jnp.dot(x, wi[e, :, h:h + tile], preferred_element_type=F32)
                hidden = jnp.maximum(hidden, 0.0).astype(BF16)
                y = y + jnp.dot(hidden, wo[e, h:h + tile, :], preferred_element_type=F32)
            y = y.astype(BF16).reshape(CHUNK, capacity, model_dim)
            back[c * CHUNK:(c + 1) * CHUNK, r, :] = y
            if self_step // CHUNK == c:
                home[self_step, r, :] = y[self_step % CHUNK]

        for k in range(c * CHUNK, (c + 1) * CHUNK):
            if k != self_step:
                home_copy[k].start()

    block = 256
    for c in range(chunks):
        for k in range(c * CHUNK, (c + 1) * CHUNK):
            if k != self_step:
                home_copy[k].wait_recv()

        @pl.loop(0, token_count // block)
        def _(i):
            r = pl.ds(pl.multiple_of(i * block, block), block)
            y = home[c * CHUNK:(c + 1) * CHUNK].reshape(span, model_dim)
            part = jnp.dot(cw[r, c * span:(c + 1) * span], y, preferred_element_type=F32)
            if c > 0:
                part = acc[r, :] + part
            if c < chunks - 1:
                acc[r, :] = part
            else:
                out_ref[r, :] = part.astype(BF16)

    for k in range(steps):
        if k != self_step:
            forth[k].wait_send()
            home_copy[k].wait_send()


def solution(mesh):
    n = mesh.shape["ep"]
    offsets = step_offsets(math.isqrt(n // 2))

    def local_layer(tokens, w_gate, expert_ids, keep_second, w_in, w_out):
        token_count, model_dim = tokens.shape[1:]
        expert_count = w_gate.shape[1]
        local_experts, _, hidden_dim = w_in.shape
        capacity = 2 * token_count // expert_count
        rows = local_experts * capacity
        any_space = pl.BlockSpec(memory_space=pl.ANY)
        vmem = pltpu.VMEM
        out = pl.pallas_call(
            functools.partial(layer_kernel, n, offsets),
            out_shape=jax.ShapeDtypeStruct((token_count, model_dim), BF16),
            in_specs=[any_space] * 6,
            out_specs=pl.BlockSpec(memory_space=vmem),
            scratch_shapes=[
                vmem((token_count, model_dim), BF16),
                vmem((expert_count, model_dim), BF16),
                vmem((2, token_count), jnp.int32),
                vmem((1, token_count), jnp.int32),
                vmem(w_in.shape, BF16),
                vmem(w_out.shape, BF16),
                vmem((CHUNK * rows, token_count), BF16),
                vmem((n, rows, model_dim), BF16),
                vmem((n, rows, model_dim), BF16),
                vmem((n, rows, model_dim), BF16),
                vmem((n, rows, model_dim), BF16),
                vmem((token_count, 128), F32),
                vmem((token_count, n * rows), BF16),
                vmem((token_count, model_dim), F32),
                pltpu.SemaphoreType.DMA((4 + 2 * local_experts,)),
                pltpu.SemaphoreType.DMA((n,)),
                pltpu.SemaphoreType.DMA((n,)),
                pltpu.SemaphoreType.DMA((n,)),
                pltpu.SemaphoreType.DMA((n,)),
            ],
            compiler_params=pltpu.CompilerParams(
                collective_id=0, has_side_effects=True, vmem_limit_bytes=60 * 1024 * 1024),
            name="moe_layer",
        )(tokens[0], w_gate.T, expert_ids[0].T, keep_second, w_in, w_out)
        return out[None]

    group_spec = P(("dp", "ep"))
    return jax.shard_map(
        local_layer, mesh=mesh, in_specs=(group_spec, P(), group_spec, group_spec, P("ep"), P("ep")),
        out_specs=group_spec, check_vma=False)
```

```python
import functools
import math

import jax
import jax.numpy as jnp
from jax import lax
from jax.experimental import pallas as pl
from jax.experimental.pallas import tpu as pltpu
from jax.sharding import PartitionSpec as P

F32 = jnp.float32
BF16 = jnp.bfloat16
MESH = pl.DeviceIdType.MESH
CHUNK = 8


def step_offsets():
    knights = [[(2, 1), (1, 2), (0, -1), (-1, 0)], [(2, -1), (-1, 2), (0, 1), (1, 0)]]
    corners = [(1, 1), (-1, -1), (1, -1), (-1, 1)]
    across = [(0, 2), (2, 0), (2, 2)]
    order = [(y, x, core) for core in range(2) for half in knights for (y, x) in half]
    order += [(y, x, core) for core in range(2) for (y, x) in corners]
    order += [(y, x, core) for core in range(2) for (y, x) in across]
    return order + [(0, 0, 1), (0, 0, 0)]


def layer_kernel(
    n, offsets, tok_hbm, wg_hbm, ids_hbm, keep_hbm, wi_hbm, wo_hbm, out_ref,
    tok, wg, ids, keep, wi, wo, onehot, send, recv, back, home, cols, cw, acc,
    local_sem, fs_sem, fr_sem, bs_sem, br_sem,
):
    side = math.isqrt(n // 2)
    token_count, model_dim = tok.shape
    expert_count = wg.shape[0]
    local_experts, _, hidden_dim = wi.shape
    steps, rows, _ = send.shape
    capacity = rows // local_experts
    chunks = steps // CHUNK
    span = CHUNK * rows
    self_step = offsets.index((0, 0, 0))

    loads = [
        pltpu.make_async_copy(src, dst, local_sem.at[i])
        for i, (src, dst) in enumerate([(ids_hbm, ids), (keep_hbm, keep), (tok_hbm, tok), (wg_hbm, wg)])
    ]
    for e in range(local_experts):
        loads.append(pltpu.make_async_copy(wi_hbm.at[e], wi.at[e], local_sem.at[4 + 2 * e]))
        loads.append(pltpu.make_async_copy(wo_hbm.at[e], wo.at[e], local_sem.at[5 + 2 * e]))
    for load in loads[:4]:
        load.start()

    barrier = pltpu.get_barrier_semaphore()

    for k in range(n):
        pl.semaphore_signal(barrier, inc=1, device_id={"ep": k}, device_id_type=MESH)

    me = lax.axis_index("ep")
    my_y, my_x, my_core = me // (2 * side), (me // 2) % side, me % 2

    def peer(step, sign):
        dy, dx, core = offsets[step]
        y, x = (my_y + sign * dy + side) % side, (my_x + sign * dx + side) % side
        return (y * side + x) * 2 + (my_core + core) % 2

    dst = [peer(k, 1) for k in range(steps)]
    src = [peer(k, -1) for k in range(steps)]

    def remote(buf_from, buf_to, ssem, rsem, k, device):
        return pltpu.make_async_remote_copy(
            src_ref=buf_from.at[k], dst_ref=buf_to.at[k], send_sem=ssem.at[k], recv_sem=rsem.at[k],
            device_id={"ep": device}, device_id_type=MESH)

    forth = [remote(send, recv, fs_sem, fr_sem, k, dst[k]) for k in range(steps)]
    home_copy = [remote(back, home, bs_sem, br_sem, k, src[k]) for k in range(steps)]

    loads[0].wait()
    loads[1].wait()
    first_id, second_id = ids[0:1, :], ids[1:2, :]
    used = keep[...] == 1
    expert_row = lax.broadcasted_iota(jnp.int32, (expert_count, token_count), 0)
    first_hot = jnp.where(expert_row == first_id, 1.0, 0.0).astype(F32)
    second_hot = jnp.where((expert_row == second_id) & used, 1.0, 0.0).astype(F32)
    first_total = jnp.sum(first_hot, axis=1, keepdims=True)
    both = jnp.concatenate([first_hot, second_hot], axis=0)
    both16 = both.astype(BF16)
    width = 256
    before = jnp.where(
        lax.broadcasted_iota(jnp.int32, (width, width), 0) < lax.broadcasted_iota(jnp.int32, (width, width), 1),
        1.0, 0.0).astype(BF16)
    carry = jnp.concatenate([jnp.zeros((expert_count, 1), F32), first_total], axis=0)
    pos = []
    for b in range(token_count // width):
        part = both[:, b * width:(b + 1) * width]
        ahead = jnp.dot(both16[:, b * width:(b + 1) * width], before, preferred_element_type=F32) + carry
        picked = part * ahead
        pos.append((jnp.sum(picked[:expert_count], axis=0, keepdims=True), jnp.sum(picked[expert_count:], axis=0, keepdims=True)))
        carry = carry + jnp.sum(part, axis=1, keepdims=True)
    pos_first = jnp.concatenate([p[0] for p in pos], axis=1).astype(jnp.int32)
    pos_second = jnp.concatenate([p[1] for p in pos], axis=1).astype(jnp.int32)
    slot_first = jnp.where(pos_first < capacity, first_id * capacity + pos_first, -1)
    slot_second = jnp.where(used & (pos_second < capacity), second_id * capacity + pos_second, -1)

    loads[2].wait()
    for c in range(chunks):
        for j in range(CHUNK):
            slot = dst[c * CHUNK + j] * rows + lax.broadcasted_iota(jnp.int32, (rows, token_count), 0)
            hit = (slot == slot_first) | (slot == slot_second)
            onehot[j * rows:(j + 1) * rows, :] = jnp.where(hit, 1.0, 0.0).astype(BF16)
        for col in range(0, model_dim, width):
            picked = jnp.dot(onehot[...], tok[:, col:col + width], preferred_element_type=F32).astype(BF16)
            for j in range(CHUNK):
                k = c * CHUNK + j
                target = recv if k == self_step else send
                target[k, :, col:col + width] = picked[j * rows:(j + 1) * rows]
        if c == 0:
            pl.semaphore_wait(barrier, n)
        for k in range(c * CHUNK, (c + 1) * CHUNK):
            if k != self_step:
                forth[k].start()
        if c == 0:
            for load in loads[4:]:
                load.start()

    loads[3].wait()
    logits = lax.dot_general(wg[...], tok[...], (((1,), (1,)), ((), ())), preferred_element_type=F32)
    top = jnp.max(logits, axis=0, keepdims=True)
    raised = jnp.exp(logits - top)
    probs = raised / jnp.sum(raised, axis=0, keepdims=True)
    expert_row = lax.broadcasted_iota(jnp.int32, (expert_count, token_count), 0)
    gate_first = jnp.sum(jnp.where(expert_row == first_id, probs, 0.0), axis=0, keepdims=True)
    gate_second = jnp.sum(jnp.where((expert_row == second_id) & used, probs, 0.0), axis=0, keepdims=True)
    gate_total = gate_first + gate_second
    lines = jnp.concatenate(
        [slot_first.astype(F32), slot_second.astype(F32), gate_first / gate_total, gate_second / gate_total,
         jnp.zeros((124, token_count), F32)], axis=0)
    cols[...] = jnp.transpose(lines)
    block = 64
    for c in range(chunks):
        lane = lax.broadcasted_iota(jnp.int32, (1, span), 1)
        slot = lane % rows
        for j in range(CHUNK):
            slot = slot + jnp.where(lane // rows == j, dst[c * CHUNK + j] * rows, 0)
        slot = slot.astype(F32)

        @pl.loop(0, token_count // block)
        def _(i):
            r = pl.ds(pl.multiple_of(i * block, block), block)
            line = cols[r, :]
            weight = jnp.where(line[:, 0:1] == slot, line[:, 2:3], 0.0) + jnp.where(line[:, 1:2] == slot, line[:, 3:4], 0.0)
            cw[r, c * span:(c + 1) * span] = weight.astype(BF16)

    for load in loads[4:]:
        load.wait()
    for c in range(chunks):
        for k in range(c * CHUNK, (c + 1) * CHUNK):
            if k != self_step:
                forth[k].wait_recv()

        @pl.loop(0, local_experts)
        def _(e):
            r = pl.ds(pl.multiple_of(e * capacity, capacity), capacity)
            x = recv[c * CHUNK:(c + 1) * CHUNK, r, :].reshape(CHUNK * capacity, model_dim)
            y = jnp.zeros((CHUNK * capacity, model_dim), F32)
            tile = 768
            for h in range(0, hidden_dim, tile):
                hidden = jnp.dot(x, wi[e, :, h:h + tile], preferred_element_type=F32)
                hidden = jnp.maximum(hidden, 0.0).astype(BF16)
                y = y + jnp.dot(hidden, wo[e, h:h + tile, :], preferred_element_type=F32)
            y = y.astype(BF16).reshape(CHUNK, capacity, model_dim)
            back[c * CHUNK:(c + 1) * CHUNK, r, :] = y
            if self_step // CHUNK == c:
                home[self_step, r, :] = y[self_step % CHUNK]

        for k in range(c * CHUNK, (c + 1) * CHUNK):
            if k != self_step:
                home_copy[k].start()

    block = 256
    pieces = [(c * CHUNK, (c + 1) * CHUNK) for c in range(chunks - 1)]
    pieces += [(steps - CHUNK, steps - CHUNK // 2), (steps - CHUNK // 2, steps)]
    for lo, hi in pieces:
        for k in range(lo, hi):
            if k != self_step:
                home_copy[k].wait_recv()

        @pl.loop(0, token_count // block)
        def _(i):
            r = pl.ds(pl.multiple_of(i * block, block), block)
            y = home[lo:hi].reshape((hi - lo) * rows, model_dim)
            part = jnp.dot(cw[r, lo * rows:hi * rows], y, preferred_element_type=F32)
            if lo > 0:
                part = acc[r, :] + part
            if hi < steps:
                acc[r, :] = part
            else:
                out_ref[r, :] = part.astype(BF16)

    for k in range(steps):
        if k != self_step:
            forth[k].wait_send()
            home_copy[k].wait_send()


def solution(mesh):
    n = mesh.shape["ep"]
    offsets = step_offsets()

    def local_layer(tokens, w_gate, expert_ids, keep_second, w_in, w_out):
        token_count, model_dim = tokens.shape[1:]
        expert_count = w_gate.shape[1]
        local_experts, _, hidden_dim = w_in.shape
        capacity = 2 * token_count // expert_count
        rows = local_experts * capacity
        any_space = pl.BlockSpec(memory_space=pltpu.HBM)
        vmem = pltpu.VMEM
        out = pl.pallas_call(
            functools.partial(layer_kernel, n, offsets),
            out_shape=jax.ShapeDtypeStruct((token_count, model_dim), BF16),
            in_specs=[any_space] * 6,
            out_specs=pl.BlockSpec(memory_space=vmem),
            scratch_shapes=[
                vmem((token_count, model_dim), BF16),
                vmem((expert_count, model_dim), BF16),
                vmem((2, token_count), jnp.int32),
                vmem((1, token_count), jnp.int32),
                vmem(w_in.shape, BF16),
                vmem(w_out.shape, BF16),
                vmem((CHUNK * rows, token_count), BF16),
                vmem((n, rows, model_dim), BF16),
                vmem((n, rows, model_dim), BF16),
                vmem((n, rows, model_dim), BF16),
                vmem((n, rows, model_dim), BF16),
                vmem((token_count, 128), F32),
                vmem((token_count, n * rows), BF16),
                vmem((token_count, model_dim), F32),
                pltpu.SemaphoreType.DMA((4 + 2 * local_experts,)),
                pltpu.SemaphoreType.DMA((n,)),
                pltpu.SemaphoreType.DMA((n,)),
                pltpu.SemaphoreType.DMA((n,)),
                pltpu.SemaphoreType.DMA((n,)),
            ],
            compiler_params=pltpu.CompilerParams(
                collective_id=0, has_side_effects=True, vmem_limit_bytes=48 * 1024 * 1024),
            name="moe_layer",
        )(*[pltpu.with_memory_space_constraint(x, pltpu.HBM)
            for x in (tokens[0], w_gate.T, expert_ids[0].T, keep_second, w_in, w_out)])
        return out[None]

    group_spec = P(("dp", "ep"))
    return jax.shard_map(
        local_layer, mesh=mesh, in_specs=(group_spec, P(), group_spec, group_spec, P("ep"), P("ep")),
        out_specs=group_spec, check_vma=False)
```

```python
import functools
import math

import jax
import jax.numpy as jnp
from jax import lax
from jax.experimental import pallas as pl
from jax.experimental.pallas import tpu as pltpu
from jax.sharding import PartitionSpec as P

F32 = jnp.float32
BF16 = jnp.bfloat16
MESH = pl.DeviceIdType.MESH
CHUNK = 8


def step_offsets():
    chunks = [
        [(2, 1), (2, -1), (0, 1), (0, -1)],
        [(1, 2), (-1, 2), (1, 0), (-1, 0)],
        [(1, 1), (-1, -1), (1, -1), (-1, 1)],
        [(0, 2), (2, 0), (2, 2)],
    ]
    order = [(y, x, core) for chunk in chunks for core in range(2) for (y, x) in chunk]
    return order + [(0, 0, 1), (0, 0, 0)]


def layer_kernel(
    n, offsets, tok_hbm, wg_hbm, ids_hbm, keep_hbm, wi_hbm, wo_hbm, out_ref,
    tok, wg, ids, keep, wi, wo, onehot, send, recv, back, home, cols, cw, acc,
    local_sem, fs_sem, fr_sem, bs_sem, br_sem,
):
    side = math.isqrt(n // 2)
    token_count, model_dim = tok.shape
    expert_count = wg.shape[0]
    local_experts, _, hidden_dim = wi.shape
    steps, rows, _ = send.shape
    capacity = rows // local_experts
    chunks = steps // CHUNK
    span = CHUNK * rows
    self_step = offsets.index((0, 0, 0))

    loads = [
        pltpu.make_async_copy(src, dst, local_sem.at[i])
        for i, (src, dst) in enumerate(
            [(ids_hbm, ids), (keep_hbm, keep), (tok_hbm, tok), (wg_hbm, wg), (wi_hbm, wi), (wo_hbm, wo)])
    ]
    for load in loads[:4]:
        load.start()

    me = lax.axis_index("ep")
    my_y, my_x, my_core = me // (2 * side), (me // 2) % side, me % 2

    def peer(step, sign):
        dy, dx, core = offsets[step]
        y, x = (my_y + sign * dy + side) % side, (my_x + sign * dx + side) % side
        return (y * side + x) * 2 + (my_core + core) % 2

    dst = [peer(k, 1) for k in range(steps)]
    src = [peer(k, -1) for k in range(steps)]

    hop = lambda d: min(d % side, -d % side)
    barrier = pltpu.get_barrier_semaphore()
    for k in sorted(range(steps - 1), key=lambda k: -hop(offsets[k][0]) - hop(offsets[k][1])):
        pl.semaphore_signal(barrier, inc=1, device_id={"ep": dst[k]}, device_id_type=MESH)

    forth_runs = [(c * CHUNK, min((c + 1) * CHUNK, steps - 1)) for c in range(chunks)]
    home_runs = forth_runs[:-1] + [(steps - CHUNK, steps - CHUNK // 2), (steps - CHUNK // 2, steps - 1)]

    def remote(buf_from, buf_to, ssem, rsem, lo, hi, run, device):
        return pltpu.make_async_remote_copy(
            src_ref=buf_from.at[lo:hi], dst_ref=buf_to.at[lo:hi], send_sem=ssem.at[0], recv_sem=rsem.at[run],
            device_id={"ep": device}, device_id_type=MESH)

    def run_of(runs, k):
        return next(i for i, (lo, hi) in enumerate(runs) if lo <= k < hi)

    def start_forth(k):
        remote(send, recv, fs_sem, fr_sem, k, k + 1, run_of(forth_runs, k), dst[k]).start()

    def start_home(k):
        remote(back, home, bs_sem, br_sem, k, k + 1, run_of(home_runs, k), src[k]).start()

    def wait_forth(run):
        remote(send, recv, fs_sem, fr_sem, *forth_runs[run], run, me).wait_recv()

    def wait_home(run):
        remote(back, home, bs_sem, br_sem, *home_runs[run], run, me).wait_recv()

    loads[0].wait()
    loads[1].wait()
    first_id, second_id = ids[0:1, :], ids[1:2, :]
    used = keep[...] == 1
    expert_row = lax.broadcasted_iota(jnp.int32, (expert_count, token_count), 0)
    first_hot = jnp.where(expert_row == first_id, 1.0, 0.0).astype(F32)
    second_hot = jnp.where((expert_row == second_id) & used, 1.0, 0.0).astype(F32)
    first_total = jnp.sum(first_hot, axis=1, keepdims=True)
    both = jnp.concatenate([first_hot, second_hot], axis=0)
    both16 = both.astype(BF16)
    width = 256
    before = jnp.where(
        lax.broadcasted_iota(jnp.int32, (width, width), 0) < lax.broadcasted_iota(jnp.int32, (width, width), 1),
        1.0, 0.0).astype(BF16)
    carry = jnp.concatenate([jnp.zeros((expert_count, 1), F32), first_total], axis=0)
    pos = []
    for b in range(token_count // width):
        part = both[:, b * width:(b + 1) * width]
        ahead = jnp.dot(both16[:, b * width:(b + 1) * width], before, preferred_element_type=F32) + carry
        picked = part * ahead
        pos.append((jnp.sum(picked[:expert_count], axis=0, keepdims=True), jnp.sum(picked[expert_count:], axis=0, keepdims=True)))
        carry = carry + jnp.sum(part, axis=1, keepdims=True)
    pos_first = jnp.concatenate([p[0] for p in pos], axis=1).astype(jnp.int32)
    pos_second = jnp.concatenate([p[1] for p in pos], axis=1).astype(jnp.int32)
    slot_first = jnp.where(pos_first < capacity, first_id * capacity + pos_first, -1)
    slot_second = jnp.where(used & (pos_second < capacity), second_id * capacity + pos_second, -1)

    loads[2].wait()
    for lo, hi in [(0, CHUNK // 2), (CHUNK // 2, CHUNK)] + [(c * CHUNK, (c + 1) * CHUNK) for c in range(1, chunks)]:
        for k in range(lo, hi):
            slot = dst[k] * rows + lax.broadcasted_iota(jnp.int32, (rows, token_count), 0)
            hit = (slot == slot_first) | (slot == slot_second)
            onehot[(k - lo) * rows:(k - lo + 1) * rows, :] = jnp.where(hit, 1.0, 0.0).astype(BF16)
        for col in range(0, model_dim, width):
            picked = jnp.dot(onehot[:(hi - lo) * rows, :], tok[:, col:col + width], preferred_element_type=F32).astype(BF16)
            for k in range(lo, hi):
                target = recv if k == self_step else send
                target[k, :, col:col + width] = picked[(k - lo) * rows:(k - lo + 1) * rows]
        if lo == 0:
            pl.semaphore_wait(barrier, n - 1)
        for k in range(lo, hi):
            if k != self_step:
                start_forth(k)
        if lo == 0:
            for load in loads[4:]:
                load.start()

    loads[3].wait()
    logits = lax.dot_general(wg[...], tok[...], (((1,), (1,)), ((), ())), preferred_element_type=F32)
    top = jnp.max(logits, axis=0, keepdims=True)
    raised = jnp.exp(logits - top)
    probs = raised / jnp.sum(raised, axis=0, keepdims=True)
    expert_row = lax.broadcasted_iota(jnp.int32, (expert_count, token_count), 0)
    gate_first = jnp.sum(jnp.where(expert_row == first_id, probs, 0.0), axis=0, keepdims=True)
    gate_second = jnp.sum(jnp.where((expert_row == second_id) & used, probs, 0.0), axis=0, keepdims=True)
    gate_total = gate_first + gate_second
    lines = jnp.concatenate(
        [slot_first.astype(F32), slot_second.astype(F32), gate_first / gate_total, gate_second / gate_total,
         jnp.zeros((124, token_count), F32)], axis=0)
    cols[...] = jnp.transpose(lines)
    block = 64
    for c in range(chunks):
        lane = lax.broadcasted_iota(jnp.int32, (1, span), 1)
        slot = lane % rows
        for j in range(CHUNK):
            slot = slot + jnp.where(lane // rows == j, dst[c * CHUNK + j] * rows, 0)
        slot = slot.astype(F32)

        @pl.loop(0, token_count // block)
        def _(i):
            r = pl.ds(pl.multiple_of(i * block, block), block)
            line = cols[r, :]
            weight = jnp.where(line[:, 0:1] == slot, line[:, 2:3], 0.0) + jnp.where(line[:, 1:2] == slot, line[:, 3:4], 0.0)
            cw[r, c * span:(c + 1) * span] = weight.astype(BF16)

    for load in loads[4:]:
        load.wait()
    for c in range(chunks):
        wait_forth(c)

        @pl.loop(0, local_experts)
        def _(e):
            r = pl.ds(pl.multiple_of(e * capacity, capacity), capacity)
            x = recv[c * CHUNK:(c + 1) * CHUNK, r, :].reshape(CHUNK * capacity, model_dim)
            y = jnp.zeros((CHUNK * capacity, model_dim), F32)
            tile = 768
            for h in range(0, hidden_dim, tile):
                hidden = jnp.dot(x, wi[e, :, h:h + tile], preferred_element_type=F32)
                hidden = jnp.maximum(hidden, 0.0).astype(BF16)
                y = y + jnp.dot(hidden, wo[e, h:h + tile, :], preferred_element_type=F32)
            y = y.astype(BF16).reshape(CHUNK, capacity, model_dim)
            back[c * CHUNK:(c + 1) * CHUNK, r, :] = y
            if self_step // CHUNK == c:
                home[self_step, r, :] = y[self_step % CHUNK]

        for k in range(c * CHUNK, (c + 1) * CHUNK):
            if k != self_step:
                start_home(k)

    block = 256
    for run, (lo, hi) in enumerate(home_runs):
        wait_home(run)
        hi = steps if hi == steps - 1 else hi

        @pl.loop(0, token_count // block)
        def _(i):
            r = pl.ds(pl.multiple_of(i * block, block), block)
            y = home[lo:hi].reshape((hi - lo) * rows, model_dim)
            part = jnp.dot(cw[r, lo * rows:hi * rows], y, preferred_element_type=F32)
            if lo > 0:
                part = acc[r, :] + part
            if hi < steps:
                acc[r, :] = part
            else:
                out_ref[r, :] = part.astype(BF16)

    remote(send, recv, fs_sem, fr_sem, 0, steps - 1, 0, me).wait_send()
    remote(back, home, bs_sem, br_sem, 0, steps - 1, 0, me).wait_send()


def solution(mesh):
    n = mesh.shape["ep"]
    offsets = step_offsets()

    def local_layer(tokens, w_gate, expert_ids, keep_second, w_in, w_out):
        token_count, model_dim = tokens.shape[1:]
        expert_count = w_gate.shape[1]
        local_experts, _, hidden_dim = w_in.shape
        capacity = 2 * token_count // expert_count
        rows = local_experts * capacity
        any_space = pl.BlockSpec(memory_space=pltpu.HBM)
        vmem = pltpu.VMEM
        out = pl.pallas_call(
            functools.partial(layer_kernel, n, offsets),
            out_shape=jax.ShapeDtypeStruct((token_count, model_dim), BF16),
            in_specs=[any_space] * 6,
            out_specs=pl.BlockSpec(memory_space=vmem),
            scratch_shapes=[
                vmem((token_count, model_dim), BF16),
                vmem((expert_count, model_dim), BF16),
                vmem((2, token_count), jnp.int32),
                vmem((1, token_count), jnp.int32),
                vmem(w_in.shape, BF16),
                vmem(w_out.shape, BF16),
                vmem((CHUNK * rows, token_count), BF16),
                vmem((n, rows, model_dim), BF16),
                vmem((n, rows, model_dim), BF16),
                vmem((n, rows, model_dim), BF16),
                vmem((n, rows, model_dim), BF16),
                vmem((token_count, 128), F32),
                vmem((token_count, n * rows), BF16),
                vmem((token_count, model_dim), F32),
                pltpu.SemaphoreType.DMA((6,)),
                pltpu.SemaphoreType.DMA((1,)),
                pltpu.SemaphoreType.DMA((n // CHUNK,)),
                pltpu.SemaphoreType.DMA((1,)),
                pltpu.SemaphoreType.DMA((n // CHUNK + 1,)),
            ],
            compiler_params=pltpu.CompilerParams(
                collective_id=0, has_side_effects=True, vmem_limit_bytes=48 * 1024 * 1024),
            name="moe_layer",
        )(*[pltpu.with_memory_space_constraint(x, pltpu.HBM)
            for x in (tokens[0], w_gate.T, expert_ids[0].T, keep_second, w_in, w_out)])
        return out[None]

    group_spec = P(("dp", "ep"))
    return jax.shard_map(
        local_layer, mesh=mesh, in_specs=(group_spec, P(), group_spec, group_spec, P("ep"), P("ep")),
        out_specs=group_spec, check_vma=False)
```

```python
import functools
import math

import jax
import jax.numpy as jnp
from jax import lax
from jax.experimental import pallas as pl
from jax.experimental.pallas import tpu as pltpu
from jax.sharding import PartitionSpec as P

F32 = jnp.float32
BF16 = jnp.bfloat16
MESH = pl.DeviceIdType.MESH
CHUNK = 8


def step_offsets():
    chunks = [
        [(2, 1), (2, -1), (0, 1), (0, -1)],
        [(1, 2), (-1, 2), (1, 0), (-1, 0)],
        [(0, 2), (2, 0), (2, 2)],
        [(1, 1), (-1, -1), (1, -1), (-1, 1)],
    ]
    order = []
    for chunk in chunks:
        order += [(y, x, core) for core in range(2) for (y, x) in chunk]
        if len(chunk) < CHUNK // 2:
            order += [(0, 0, 1), (0, 0, 0)]
    return order


def layer_kernel(
    n, offsets, tok_hbm, wg_hbm, ids_hbm, keep_hbm, wi_hbm, wo_hbm, out_ref,
    tok, wg, ids, keep, wi, wo, onehot, send, recv, back, home, cols, cw, acc,
    local_sem, fs_sem, fr_sem, bs_sem, br_sem,
):
    side = math.isqrt(n // 2)
    token_count, model_dim = tok.shape
    expert_count = wg.shape[0]
    local_experts, _, hidden_dim = wi.shape
    steps, rows, _ = send.shape
    capacity = rows // local_experts
    chunks = steps // CHUNK
    span = CHUNK * rows
    self_step = offsets.index((0, 0, 0))

    loads = [
        pltpu.make_async_copy(src, dst, local_sem.at[i])
        for i, (src, dst) in enumerate(
            [(ids_hbm, ids), (keep_hbm, keep), (tok_hbm, tok), (wg_hbm, wg), (wi_hbm, wi), (wo_hbm, wo)])
    ]
    for load in loads[:4]:
        load.start()

    me = lax.axis_index("ep")
    my_y, my_x, my_core = me // (2 * side), (me // 2) % side, me % 2

    def peer(step, sign):
        dy, dx, core = offsets[step]
        y, x = (my_y + sign * dy + side) % side, (my_x + sign * dx + side) % side
        return (y * side + x) * 2 + (my_core + core) % 2

    dst = [peer(k, 1) for k in range(steps)]
    src = [peer(k, -1) for k in range(steps)]

    hop = lambda d: min(d % side, -d % side)
    barrier = pltpu.get_barrier_semaphore()
    peers = [k for k in range(steps) if k != self_step]
    for k in sorted(peers, key=lambda k: -hop(offsets[k][0]) - hop(offsets[k][1])):
        pl.semaphore_signal(barrier, inc=1, device_id={"ep": dst[k]}, device_id_type=MESH)

    forth_runs = [(c * CHUNK, (c + 1) * CHUNK) for c in range(chunks)]
    home_runs = forth_runs[:-1] + [(steps - CHUNK, steps - CHUNK // 2), (steps - CHUNK // 2, steps)]

    def travel(lo, hi):
        return lo, hi - 1 if hi - 1 == self_step else hi

    def remote(buf_from, buf_to, ssem, rsem, lo, hi, run, device):
        return pltpu.make_async_remote_copy(
            src_ref=buf_from.at[lo:hi], dst_ref=buf_to.at[lo:hi], send_sem=ssem.at[0], recv_sem=rsem.at[run],
            device_id={"ep": device}, device_id_type=MESH)

    def run_of(runs, k):
        return next(i for i, (lo, hi) in enumerate(runs) if lo <= k < hi)

    def start_forth(k):
        remote(send, recv, fs_sem, fr_sem, k, k + 1, run_of(forth_runs, k), dst[k]).start()

    def start_home(k):
        remote(back, home, bs_sem, br_sem, k, k + 1, run_of(home_runs, k), src[k]).start()

    def wait_forth(run):
        remote(send, recv, fs_sem, fr_sem, *travel(*forth_runs[run]), run, me).wait_recv()

    def wait_home(run):
        remote(back, home, bs_sem, br_sem, *travel(*home_runs[run]), run, me).wait_recv()

    loads[0].wait()
    loads[1].wait()
    first_id, second_id = ids[0:1, :], ids[1:2, :]
    used = keep[...] == 1
    expert_row = lax.broadcasted_iota(jnp.int32, (expert_count, token_count), 0)
    first_hot = jnp.where(expert_row == first_id, 1.0, 0.0).astype(F32)
    second_hot = jnp.where((expert_row == second_id) & used, 1.0, 0.0).astype(F32)
    first_total = jnp.sum(first_hot, axis=1, keepdims=True)
    both = jnp.concatenate([first_hot, second_hot], axis=0)
    both16 = both.astype(BF16)
    width = 256
    before = jnp.where(
        lax.broadcasted_iota(jnp.int32, (width, width), 0) < lax.broadcasted_iota(jnp.int32, (width, width), 1),
        1.0, 0.0).astype(BF16)
    carry = jnp.concatenate([jnp.zeros((expert_count, 1), F32), first_total], axis=0)
    pos = []
    for b in range(token_count // width):
        part = both[:, b * width:(b + 1) * width]
        ahead = jnp.dot(both16[:, b * width:(b + 1) * width], before, preferred_element_type=F32) + carry
        picked = part * ahead
        pos.append((jnp.sum(picked[:expert_count], axis=0, keepdims=True), jnp.sum(picked[expert_count:], axis=0, keepdims=True)))
        carry = carry + jnp.sum(part, axis=1, keepdims=True)
    pos_first = jnp.concatenate([p[0] for p in pos], axis=1).astype(jnp.int32)
    pos_second = jnp.concatenate([p[1] for p in pos], axis=1).astype(jnp.int32)
    slot_first = jnp.where(pos_first < capacity, first_id * capacity + pos_first, -1)
    slot_second = jnp.where(used & (pos_second < capacity), second_id * capacity + pos_second, -1)

    loads[2].wait()
    for lo, hi in [(0, CHUNK // 2), (CHUNK // 2, CHUNK)] + [(c * CHUNK, (c + 1) * CHUNK) for c in range(1, chunks)]:
        for k in range(lo, hi):
            slot = dst[k] * rows + lax.broadcasted_iota(jnp.int32, (rows, token_count), 0)
            hit = (slot == slot_first) | (slot == slot_second)
            onehot[(k - lo) * rows:(k - lo + 1) * rows, :] = jnp.where(hit, 1.0, 0.0).astype(BF16)
        for col in range(0, model_dim, width):
            picked = jnp.dot(onehot[:(hi - lo) * rows, :], tok[:, col:col + width], preferred_element_type=F32).astype(BF16)
            for k in range(lo, hi):
                target = recv if k == self_step else send
                target[k, :, col:col + width] = picked[(k - lo) * rows:(k - lo + 1) * rows]
        if lo == 0:
            pl.semaphore_wait(barrier, n - 1)
        for k in range(lo, hi):
            if k != self_step:
                start_forth(k)
        if lo == 0:
            for load in loads[4:]:
                load.start()

    loads[3].wait()
    logits = lax.dot_general(wg[...], tok[...], (((1,), (1,)), ((), ())), preferred_element_type=F32)
    top = jnp.max(logits, axis=0, keepdims=True)
    raised = jnp.exp(logits - top)
    probs = raised / jnp.sum(raised, axis=0, keepdims=True)
    expert_row = lax.broadcasted_iota(jnp.int32, (expert_count, token_count), 0)
    gate_first = jnp.sum(jnp.where(expert_row == first_id, probs, 0.0), axis=0, keepdims=True)
    gate_second = jnp.sum(jnp.where((expert_row == second_id) & used, probs, 0.0), axis=0, keepdims=True)
    gate_total = gate_first + gate_second
    lines = jnp.concatenate(
        [slot_first.astype(F32), slot_second.astype(F32), gate_first / gate_total, gate_second / gate_total,
         jnp.zeros((124, token_count), F32)], axis=0)
    cols[...] = jnp.transpose(lines)
    block = 64
    for c in range(chunks):
        lane = lax.broadcasted_iota(jnp.int32, (1, span), 1)
        slot = lane % rows
        for j in range(CHUNK):
            slot = slot + jnp.where(lane // rows == j, dst[c * CHUNK + j] * rows, 0)
        slot = slot.astype(F32)

        @pl.loop(0, token_count // block)
        def _(i):
            r = pl.ds(pl.multiple_of(i * block, block), block)
            line = cols[r, :]
            weight = jnp.where(line[:, 0:1] == slot, line[:, 2:3], 0.0) + jnp.where(line[:, 1:2] == slot, line[:, 3:4], 0.0)
            cw[r, c * span:(c + 1) * span] = weight.astype(BF16)

    for load in loads[4:]:
        load.wait()
    for c in range(chunks):
        wait_forth(c)

        @pl.loop(0, local_experts)
        def _(e):
            r = pl.ds(pl.multiple_of(e * capacity, capacity), capacity)
            x = recv[c * CHUNK:(c + 1) * CHUNK, r, :].reshape(CHUNK * capacity, model_dim)
            y = jnp.zeros((CHUNK * capacity, model_dim), F32)
            tile = 768
            for h in range(0, hidden_dim, tile):
                hidden = jnp.dot(x, wi[e, :, h:h + tile], preferred_element_type=F32)
                hidden = jnp.maximum(hidden, 0.0).astype(BF16)
                y = y + jnp.dot(hidden, wo[e, h:h + tile, :], preferred_element_type=F32)
            y = y.astype(BF16).reshape(CHUNK, capacity, model_dim)
            back[c * CHUNK:(c + 1) * CHUNK, r, :] = y
            if self_step // CHUNK == c:
                home[self_step, r, :] = y[self_step % CHUNK]

        for k in range(c * CHUNK, (c + 1) * CHUNK):
            if k != self_step:
                start_home(k)

    block = 256
    for run, (lo, hi) in enumerate(home_runs):
        wait_home(run)

        @pl.loop(0, token_count // block)
        def _(i):
            r = pl.ds(pl.multiple_of(i * block, block), block)
            y = home[lo:hi].reshape((hi - lo) * rows, model_dim)
            part = jnp.dot(cw[r, lo * rows:hi * rows], y, preferred_element_type=F32)
            if lo > 0:
                part = acc[r, :] + part
            if hi < steps:
                acc[r, :] = part
            else:
                out_ref[r, :] = part.astype(BF16)

    for lo, hi in ((0, self_step), (self_step + 1, steps)):
        if lo < hi:
            remote(send, recv, fs_sem, fr_sem, lo, hi, 0, me).wait_send()
            remote(back, home, bs_sem, br_sem, lo, hi, 0, me).wait_send()


def solution(mesh):
    n = mesh.shape["ep"]
    offsets = step_offsets()

    def local_layer(tokens, w_gate, expert_ids, keep_second, w_in, w_out):
        token_count, model_dim = tokens.shape[1:]
        expert_count = w_gate.shape[1]
        local_experts, _, hidden_dim = w_in.shape
        capacity = 2 * token_count // expert_count
        rows = local_experts * capacity
        any_space = pl.BlockSpec(memory_space=pltpu.HBM)
        vmem = pltpu.VMEM
        out = pl.pallas_call(
            functools.partial(layer_kernel, n, offsets),
            out_shape=jax.ShapeDtypeStruct((token_count, model_dim), BF16),
            in_specs=[any_space] * 6,
            out_specs=pl.BlockSpec(memory_space=vmem),
            scratch_shapes=[
                vmem((token_count, model_dim), BF16),
                vmem((expert_count, model_dim), BF16),
                vmem((2, token_count), jnp.int32),
                vmem((1, token_count), jnp.int32),
                vmem(w_in.shape, BF16),
                vmem(w_out.shape, BF16),
                vmem((CHUNK * rows, token_count), BF16),
                vmem((n, rows, model_dim), BF16),
                vmem((n, rows, model_dim), BF16),
                vmem((n, rows, model_dim), BF16),
                vmem((n, rows, model_dim), BF16),
                vmem((token_count, 128), F32),
                vmem((token_count, n * rows), BF16),
                vmem((token_count, model_dim), F32),
                pltpu.SemaphoreType.DMA((6,)),
                pltpu.SemaphoreType.DMA((1,)),
                pltpu.SemaphoreType.DMA((n // CHUNK,)),
                pltpu.SemaphoreType.DMA((1,)),
                pltpu.SemaphoreType.DMA((n // CHUNK + 1,)),
            ],
            compiler_params=pltpu.CompilerParams(
                collective_id=0, has_side_effects=True, vmem_limit_bytes=48 * 1024 * 1024),
            name="moe_layer",
        )(*[pltpu.with_memory_space_constraint(x, pltpu.HBM)
            for x in (tokens[0], w_gate.T, expert_ids[0].T, keep_second, w_in, w_out)])
        return out[None]

    group_spec = P(("dp", "ep"))
    return jax.shard_map(
        local_layer, mesh=mesh, in_specs=(group_spec, P(), group_spec, group_spec, P("ep"), P("ep")),
        out_specs=group_spec, check_vma=False)
```

```python
import functools
import math

import jax
import jax.numpy as jnp
from jax import lax
from jax.experimental import pallas as pl
from jax.experimental.pallas import tpu as pltpu
from jax.sharding import PartitionSpec as P

F32 = jnp.float32
BF16 = jnp.bfloat16
MESH = pl.DeviceIdType.MESH
CHUNK = 8


def step_offsets():
    chunks = [
        [(1, 1), (-1, -1), (1, -1), (-1, 1)],
        [(2, 1), (2, -1), (0, 1), (0, -1)],
        [(1, 2), (-1, 2), (1, 0), (-1, 0)],
        [(0, 2), (2, 0), (2, 2)],
    ]
    order = []
    for chunk in chunks:
        order += [(y, x, core) for core in range(2) for (y, x) in chunk]
        if len(chunk) < CHUNK // 2:
            order += [(0, 0, 1), (0, 0, 0)]
    return order


def layer_kernel(
    n, offsets, tok_hbm, wg_hbm, ids_hbm, keep_hbm, wi_hbm, wo_hbm, out_ref,
    tok, wg, ids, keep, wi, wo, onehot, send, recv, back, home, cols, cw, acc,
    ready_sem, local_sem, fs_sem, fr_sem, bs_sem, br_sem,
):
    side = math.isqrt(n // 2)
    token_count, model_dim = tok.shape
    expert_count = wg.shape[0]
    local_experts, _, hidden_dim = wi.shape
    steps, rows, _ = send.shape
    capacity = rows // local_experts
    chunks = steps // CHUNK
    span = CHUNK * rows
    self_step = offsets.index((0, 0, 0))

    loads = [
        pltpu.make_async_copy(src, dst, local_sem.at[i])
        for i, (src, dst) in enumerate(
            [(ids_hbm, ids), (keep_hbm, keep), (tok_hbm, tok), (wg_hbm, wg), (wi_hbm, wi), (wo_hbm, wo)])
    ]
    for load in loads[:4]:
        load.start()

    me = lax.axis_index("ep")
    my_y, my_x, my_core = me // (2 * side), (me // 2) % side, me % 2

    def peer(step, sign):
        dy, dx, core = offsets[step]
        y, x = (my_y + sign * dy + side) % side, (my_x + sign * dx + side) % side
        return (y * side + x) * 2 + (my_core + core) % 2

    dst = [peer(k, 1) for k in range(steps)]
    src = [peer(k, -1) for k in range(steps)]

    hop = lambda d: min(d % side, -d % side)
    peers = [k for k in range(steps) if k != self_step]
    near = [k for k in peers if hop(offsets[k][0]) + hop(offsets[k][1]) <= 2]
    assert all(k in near for k in range(CHUNK))
    barrier = pltpu.get_barrier_semaphore()
    for k in sorted(near, key=lambda k: -hop(offsets[k][0]) - hop(offsets[k][1])):
        pl.semaphore_signal(barrier, inc=1, device_id={"ep": dst[k]}, device_id_type=MESH)

    forth_runs = [(c * CHUNK, (c + 1) * CHUNK) for c in range(chunks)]
    home_runs = forth_runs[:-1] + [(steps - CHUNK, steps - CHUNK // 2), (steps - CHUNK // 2, steps)]

    def travel(lo, hi):
        return lo, hi - 1 if hi - 1 == self_step else hi

    def remote(buf_from, buf_to, ssem, rsem, lo, hi, run, device):
        return pltpu.make_async_remote_copy(
            src_ref=buf_from.at[lo:hi], dst_ref=buf_to.at[lo:hi], send_sem=ssem.at[0], recv_sem=rsem.at[run],
            device_id={"ep": device}, device_id_type=MESH)

    def run_of(runs, k):
        return next(i for i, (lo, hi) in enumerate(runs) if lo <= k < hi)

    def start_forth(k):
        remote(send, recv, fs_sem, fr_sem, k, k + 1, run_of(forth_runs, k), dst[k]).start()

    def start_home(k):
        remote(back, home, bs_sem, br_sem, k, k + 1, run_of(home_runs, k), src[k]).start()

    def wait_forth(run):
        remote(send, recv, fs_sem, fr_sem, *travel(*forth_runs[run]), run, me).wait_recv()

    def wait_home(run):
        remote(back, home, bs_sem, br_sem, *travel(*home_runs[run]), run, me).wait_recv()

    loads[0].wait()
    loads[1].wait()
    first_id, second_id = ids[0:1, :], ids[1:2, :]
    used = keep[...] == 1
    expert_row = lax.broadcasted_iota(jnp.int32, (expert_count, token_count), 0)
    first_hot = jnp.where(expert_row == first_id, 1.0, 0.0).astype(F32)
    second_hot = jnp.where((expert_row == second_id) & used, 1.0, 0.0).astype(F32)
    first_total = jnp.sum(first_hot, axis=1, keepdims=True)
    both = jnp.concatenate([first_hot, second_hot], axis=0)
    both16 = both.astype(BF16)
    width = 256
    before = jnp.where(
        lax.broadcasted_iota(jnp.int32, (width, width), 0) < lax.broadcasted_iota(jnp.int32, (width, width), 1),
        1.0, 0.0).astype(BF16)
    carry = jnp.concatenate([jnp.zeros((expert_count, 1), F32), first_total], axis=0)
    pos = []
    for b in range(token_count // width):
        part = both[:, b * width:(b + 1) * width]
        ahead = jnp.dot(both16[:, b * width:(b + 1) * width], before, preferred_element_type=F32) + carry
        picked = part * ahead
        pos.append((jnp.sum(picked[:expert_count], axis=0, keepdims=True), jnp.sum(picked[expert_count:], axis=0, keepdims=True)))
        carry = carry + jnp.sum(part, axis=1, keepdims=True)
    pos_first = jnp.concatenate([p[0] for p in pos], axis=1).astype(jnp.int32)
    pos_second = jnp.concatenate([p[1] for p in pos], axis=1).astype(jnp.int32)
    slot_first = jnp.where(pos_first < capacity, first_id * capacity + pos_first, -1)
    slot_second = jnp.where(used & (pos_second < capacity), second_id * capacity + pos_second, -1)

    pl.semaphore_wait(barrier, len(near))
    for k in near:
        pl.semaphore_signal(ready_sem, inc=1, device_id={"ep": dst[k]}, device_id_type=MESH)

    loads[2].wait()
    for lo, hi in [(0, CHUNK // 2), (CHUNK // 2, CHUNK)] + [(c * CHUNK, (c + 1) * CHUNK) for c in range(1, chunks)]:
        for k in range(lo, hi):
            slot = dst[k] * rows + lax.broadcasted_iota(jnp.int32, (rows, token_count), 0)
            hit = (slot == slot_first) | (slot == slot_second)
            onehot[(k - lo) * rows:(k - lo + 1) * rows, :] = jnp.where(hit, 1.0, 0.0).astype(BF16)
        for col in range(0, model_dim, width):
            picked = jnp.dot(onehot[:(hi - lo) * rows, :], tok[:, col:col + width], preferred_element_type=F32).astype(BF16)
            for k in range(lo, hi):
                target = recv if k == self_step else send
                target[k, :, col:col + width] = picked[(k - lo) * rows:(k - lo + 1) * rows]
        if lo == CHUNK:
            pl.semaphore_wait(ready_sem, len(near))
        for k in range(lo, hi):
            if k != self_step:
                start_forth(k)
        if lo == 0:
            for load in loads[4:]:
                load.start()

    loads[3].wait()
    logits = lax.dot_general(wg[...], tok[...], (((1,), (1,)), ((), ())), preferred_element_type=F32)
    top = jnp.max(logits, axis=0, keepdims=True)
    raised = jnp.exp(logits - top)
    probs = raised / jnp.sum(raised, axis=0, keepdims=True)
    expert_row = lax.broadcasted_iota(jnp.int32, (expert_count, token_count), 0)
    gate_first = jnp.sum(jnp.where(expert_row == first_id, probs, 0.0), axis=0, keepdims=True)
    gate_second = jnp.sum(jnp.where((expert_row == second_id) & used, probs, 0.0), axis=0, keepdims=True)
    gate_total = gate_first + gate_second
    lines = jnp.concatenate(
        [slot_first.astype(F32), slot_second.astype(F32), gate_first / gate_total, gate_second / gate_total,
         jnp.zeros((124, token_count), F32)], axis=0)
    cols[...] = jnp.transpose(lines)
    block = 64
    for c in range(chunks):
        lane = lax.broadcasted_iota(jnp.int32, (1, span), 1)
        slot = lane % rows
        for j in range(CHUNK):
            slot = slot + jnp.where(lane // rows == j, dst[c * CHUNK + j] * rows, 0)
        slot = slot.astype(F32)

        @pl.loop(0, token_count // block)
        def _(i):
            r = pl.ds(pl.multiple_of(i * block, block), block)
            line = cols[r, :]
            weight = jnp.where(line[:, 0:1] == slot, line[:, 2:3], 0.0) + jnp.where(line[:, 1:2] == slot, line[:, 3:4], 0.0)
            cw[r, c * span:(c + 1) * span] = weight.astype(BF16)

    for load in loads[4:]:
        load.wait()
    for c in range(chunks):
        wait_forth(c)

        @pl.loop(0, local_experts)
        def _(e):
            r = pl.ds(pl.multiple_of(e * capacity, capacity), capacity)
            x = recv[c * CHUNK:(c + 1) * CHUNK, r, :].reshape(CHUNK * capacity, model_dim)
            y = jnp.zeros((CHUNK * capacity, model_dim), F32)
            tile = 768
            for h in range(0, hidden_dim, tile):
                hidden = jnp.dot(x, wi[e, :, h:h + tile], preferred_element_type=F32)
                hidden = jnp.maximum(hidden, 0.0).astype(BF16)
                y = y + jnp.dot(hidden, wo[e, h:h + tile, :], preferred_element_type=F32)
            y = y.astype(BF16).reshape(CHUNK, capacity, model_dim)
            back[c * CHUNK:(c + 1) * CHUNK, r, :] = y
            if self_step // CHUNK == c:
                home[self_step, r, :] = y[self_step % CHUNK]

        for k in range(c * CHUNK, (c + 1) * CHUNK):
            if k != self_step:
                start_home(k)

    block = 256
    for run, (lo, hi) in enumerate(home_runs):
        wait_home(run)

        @pl.loop(0, token_count // block)
        def _(i):
            r = pl.ds(pl.multiple_of(i * block, block), block)
            y = home[lo:hi].reshape((hi - lo) * rows, model_dim)
            part = jnp.dot(cw[r, lo * rows:hi * rows], y, preferred_element_type=F32)
            if lo > 0:
                part = acc[r, :] + part
            if hi < steps:
                acc[r, :] = part
            else:
                out_ref[r, :] = part.astype(BF16)

    for lo, hi in ((0, self_step), (self_step + 1, steps)):
        if lo < hi:
            remote(send, recv, fs_sem, fr_sem, lo, hi, 0, me).wait_send()
            remote(back, home, bs_sem, br_sem, lo, hi, 0, me).wait_send()


def solution(mesh):
    n = mesh.shape["ep"]
    offsets = step_offsets()

    def local_layer(tokens, w_gate, expert_ids, keep_second, w_in, w_out):
        token_count, model_dim = tokens.shape[1:]
        expert_count = w_gate.shape[1]
        local_experts, _, hidden_dim = w_in.shape
        capacity = 2 * token_count // expert_count
        rows = local_experts * capacity
        any_space = pl.BlockSpec(memory_space=pltpu.HBM)
        vmem = pltpu.VMEM
        out = pl.pallas_call(
            functools.partial(layer_kernel, n, offsets),
            out_shape=jax.ShapeDtypeStruct((token_count, model_dim), BF16),
            in_specs=[any_space] * 6,
            out_specs=pl.BlockSpec(memory_space=vmem),
            scratch_shapes=[
                vmem((token_count, model_dim), BF16),
                vmem((expert_count, model_dim), BF16),
                vmem((2, token_count), jnp.int32),
                vmem((1, token_count), jnp.int32),
                vmem(w_in.shape, BF16),
                vmem(w_out.shape, BF16),
                vmem((CHUNK * rows, token_count), BF16),
                vmem((n, rows, model_dim), BF16),
                vmem((n, rows, model_dim), BF16),
                vmem((n, rows, model_dim), BF16),
                vmem((n, rows, model_dim), BF16),
                vmem((token_count, 128), F32),
                vmem((token_count, n * rows), BF16),
                vmem((token_count, model_dim), F32),
                pltpu.SemaphoreType.REGULAR,
                pltpu.SemaphoreType.DMA((6,)),
                pltpu.SemaphoreType.DMA((1,)),
                pltpu.SemaphoreType.DMA((n // CHUNK,)),
                pltpu.SemaphoreType.DMA((1,)),
                pltpu.SemaphoreType.DMA((n // CHUNK + 1,)),
            ],
            compiler_params=pltpu.CompilerParams(
                collective_id=0, has_side_effects=True, vmem_limit_bytes=48 * 1024 * 1024),
            name="moe_layer",
        )(*[pltpu.with_memory_space_constraint(x, pltpu.HBM)
            for x in (tokens[0], w_gate.T, expert_ids[0].T, keep_second, w_in, w_out)])
        return out[None]

    group_spec = P(("dp", "ep"))
    return jax.shard_map(
        local_layer, mesh=mesh, in_specs=(group_spec, P(), group_spec, group_spec, P("ep"), P("ep")),
        out_specs=group_spec, check_vma=False)
```

```python
import functools
import math

import jax
import jax.numpy as jnp
from jax import lax
from jax.experimental import pallas as pl
from jax.experimental.pallas import tpu as pltpu
from jax.sharding import PartitionSpec as P

F32 = jnp.float32
BF16 = jnp.bfloat16
MESH = pl.DeviceIdType.MESH
CHUNK = 8


def step_offsets():
    chunks = [
        [(0, 1), (0, -1), (1, 0), (-1, 0)],
        [(1, 1), (-1, -1), (1, -1), (-1, 1)],
        [(0, 2), (2, 0), (2, 2)],
        [(2, 1), (1, 2), (2, -1), (-1, 2)],
    ]
    order = []
    for chunk in chunks:
        order += [(y, x, core) for core in range(2) for (y, x) in chunk]
        if len(chunk) < CHUNK // 2:
            order += [(0, 0, 1), (0, 0, 0)]
    return order


def layer_kernel(
    n, offsets, tok_hbm, wg_hbm, ids_hbm, keep_hbm, wi_hbm, wo_hbm, out_ref,
    tok, wg, ids, keep, wi, wo, onehot, send, recv, back, home, cols, cw, acc,
    ready_sem, local_sem, fs_sem, fr_sem, bs_sem, br_sem,
):
    side = math.isqrt(n // 2)
    token_count, model_dim = tok.shape
    expert_count = wg.shape[0]
    local_experts, _, hidden_dim = wi.shape
    steps, rows, _ = send.shape
    capacity = rows // local_experts
    chunks = steps // CHUNK
    span = CHUNK * rows
    self_step = offsets.index((0, 0, 0))

    loads = [
        pltpu.make_async_copy(src, dst, local_sem.at[i])
        for i, (src, dst) in enumerate(
            [(ids_hbm, ids), (keep_hbm, keep), (tok_hbm, tok), (wg_hbm, wg), (wi_hbm, wi), (wo_hbm, wo)])
    ]
    for load in loads[:4]:
        load.start()

    me = lax.axis_index("ep")
    my_y, my_x, my_core = me // (2 * side), (me // 2) % side, me % 2

    def peer(step, sign):
        dy, dx, core = offsets[step]
        y, x = (my_y + sign * dy + side) % side, (my_x + sign * dx + side) % side
        return (y * side + x) * 2 + (my_core + core) % 2

    dst = [peer(k, 1) for k in range(steps)]
    src = [peer(k, -1) for k in range(steps)]

    hop = lambda d: min(d % side, -d % side)
    peers = [k for k in range(steps) if k != self_step]
    near = [k for k in peers if hop(offsets[k][0]) + hop(offsets[k][1]) <= 2]
    assert all(k in near for k in range(CHUNK))
    barrier = pltpu.get_barrier_semaphore()
    for k in sorted(near, key=lambda k: -hop(offsets[k][0]) - hop(offsets[k][1])):
        pl.semaphore_signal(barrier, inc=1, device_id={"ep": dst[k]}, device_id_type=MESH)

    forth_runs = [(c * CHUNK, (c + 1) * CHUNK) for c in range(chunks)]
    home_runs = forth_runs[:-1] + [(steps - CHUNK, steps - CHUNK // 2), (steps - CHUNK // 2, steps)]

    def travel(lo, hi):
        return lo, hi - 1 if hi - 1 == self_step else hi

    def remote(buf_from, buf_to, ssem, rsem, lo, hi, run, device):
        return pltpu.make_async_remote_copy(
            src_ref=buf_from.at[lo:hi], dst_ref=buf_to.at[lo:hi], send_sem=ssem.at[0], recv_sem=rsem.at[run],
            device_id={"ep": device}, device_id_type=MESH)

    def run_of(runs, k):
        return next(i for i, (lo, hi) in enumerate(runs) if lo <= k < hi)

    def start_forth(k):
        remote(send, recv, fs_sem, fr_sem, k, k + 1, run_of(forth_runs, k), dst[k]).start()

    def start_home(k):
        remote(back, home, bs_sem, br_sem, k, k + 1, run_of(home_runs, k), src[k]).start()

    def wait_forth(run):
        remote(send, recv, fs_sem, fr_sem, *travel(*forth_runs[run]), run, me).wait_recv()

    def wait_home(run):
        remote(back, home, bs_sem, br_sem, *travel(*home_runs[run]), run, me).wait_recv()

    loads[0].wait()
    loads[1].wait()
    first_id, second_id = ids[0:1, :], ids[1:2, :]
    used = keep[...] == 1
    expert_row = lax.broadcasted_iota(jnp.int32, (expert_count, token_count), 0)
    first_hot = jnp.where(expert_row == first_id, 1.0, 0.0).astype(F32)
    second_hot = jnp.where((expert_row == second_id) & used, 1.0, 0.0).astype(F32)
    first_total = jnp.sum(first_hot, axis=1, keepdims=True)
    both = jnp.concatenate([first_hot, second_hot], axis=0)
    both16 = both.astype(BF16)
    width = 256
    before = jnp.where(
        lax.broadcasted_iota(jnp.int32, (width, width), 0) < lax.broadcasted_iota(jnp.int32, (width, width), 1),
        1.0, 0.0).astype(BF16)
    carry = jnp.concatenate([jnp.zeros((expert_count, 1), F32), first_total], axis=0)
    pos = []
    for b in range(token_count // width):
        part = both[:, b * width:(b + 1) * width]
        ahead = jnp.dot(both16[:, b * width:(b + 1) * width], before, preferred_element_type=F32) + carry
        picked = part * ahead
        pos.append((jnp.sum(picked[:expert_count], axis=0, keepdims=True), jnp.sum(picked[expert_count:], axis=0, keepdims=True)))
        carry = carry + jnp.sum(part, axis=1, keepdims=True)
    pos_first = jnp.concatenate([p[0] for p in pos], axis=1).astype(jnp.int32)
    pos_second = jnp.concatenate([p[1] for p in pos], axis=1).astype(jnp.int32)
    slot_first = jnp.where(pos_first < capacity, first_id * capacity + pos_first, -1)
    slot_second = jnp.where(used & (pos_second < capacity), second_id * capacity + pos_second, -1)

    pl.semaphore_wait(barrier, len(near))
    for k in near:
        pl.semaphore_signal(ready_sem, inc=1, device_id={"ep": dst[k]}, device_id_type=MESH)

    loads[2].wait()
    for lo, hi in [(0, CHUNK // 2), (CHUNK // 2, CHUNK)] + [(c * CHUNK, (c + 1) * CHUNK) for c in range(1, chunks)]:
        for k in range(lo, hi):
            slot = dst[k] * rows + lax.broadcasted_iota(jnp.int32, (rows, token_count), 0)
            hit = (slot == slot_first) | (slot == slot_second)
            onehot[(k - lo) * rows:(k - lo + 1) * rows, :] = jnp.where(hit, 1.0, 0.0).astype(BF16)
        for col in range(0, model_dim, width):
            picked = jnp.dot(onehot[:(hi - lo) * rows, :], tok[:, col:col + width], preferred_element_type=F32).astype(BF16)
            for k in range(lo, hi):
                target = recv if k == self_step else send
                target[k, :, col:col + width] = picked[(k - lo) * rows:(k - lo + 1) * rows]
        if lo == CHUNK:
            pl.semaphore_wait(ready_sem, len(near))
        for k in range(lo, hi):
            if k != self_step:
                start_forth(k)
        if lo == 0:
            for load in loads[4:]:
                load.start()

    loads[3].wait()
    logits = lax.dot_general(wg[...], tok[...], (((1,), (1,)), ((), ())), preferred_element_type=F32)
    top = jnp.max(logits, axis=0, keepdims=True)
    raised = jnp.exp(logits - top)
    probs = raised / jnp.sum(raised, axis=0, keepdims=True)
    expert_row = lax.broadcasted_iota(jnp.int32, (expert_count, token_count), 0)
    gate_first = jnp.sum(jnp.where(expert_row == first_id, probs, 0.0), axis=0, keepdims=True)
    gate_second = jnp.sum(jnp.where((expert_row == second_id) & used, probs, 0.0), axis=0, keepdims=True)
    gate_total = gate_first + gate_second
    lines = jnp.concatenate(
        [slot_first.astype(F32), slot_second.astype(F32), gate_first / gate_total, gate_second / gate_total,
         jnp.zeros((124, token_count), F32)], axis=0)
    cols[...] = jnp.transpose(lines)
    block = 64
    for c in range(chunks):
        lane = lax.broadcasted_iota(jnp.int32, (1, span), 1)
        slot = lane % rows
        for j in range(CHUNK):
            slot = slot + jnp.where(lane // rows == j, dst[c * CHUNK + j] * rows, 0)
        slot = slot.astype(F32)

        @pl.loop(0, token_count // block)
        def _(i):
            r = pl.ds(pl.multiple_of(i * block, block), block)
            line = cols[r, :]
            weight = jnp.where(line[:, 0:1] == slot, line[:, 2:3], 0.0) + jnp.where(line[:, 1:2] == slot, line[:, 3:4], 0.0)
            cw[r, c * span:(c + 1) * span] = weight.astype(BF16)

    for load in loads[4:]:
        load.wait()
    for c in range(chunks):
        wait_forth(c)

        @pl.loop(0, local_experts)
        def _(e):
            r = pl.ds(pl.multiple_of(e * capacity, capacity), capacity)
            x = recv[c * CHUNK:(c + 1) * CHUNK, r, :].reshape(CHUNK * capacity, model_dim)
            y = jnp.zeros((CHUNK * capacity, model_dim), F32)
            tile = 768
            for h in range(0, hidden_dim, tile):
                hidden = jnp.dot(x, wi[e, :, h:h + tile], preferred_element_type=F32)
                hidden = jnp.maximum(hidden, 0.0).astype(BF16)
                y = y + jnp.dot(hidden, wo[e, h:h + tile, :], preferred_element_type=F32)
            y = y.astype(BF16).reshape(CHUNK, capacity, model_dim)
            back[c * CHUNK:(c + 1) * CHUNK, r, :] = y
            if self_step // CHUNK == c:
                home[self_step, r, :] = y[self_step % CHUNK]

        for k in range(c * CHUNK, (c + 1) * CHUNK):
            if k != self_step:
                start_home(k)

    block = 256
    for run, (lo, hi) in enumerate(home_runs):
        wait_home(run)

        @pl.loop(0, token_count // block)
        def _(i):
            r = pl.ds(pl.multiple_of(i * block, block), block)
            y = home[lo:hi].reshape((hi - lo) * rows, model_dim)
            part = jnp.dot(cw[r, lo * rows:hi * rows], y, preferred_element_type=F32)
            if lo > 0:
                part = acc[r, :] + part
            if hi < steps:
                acc[r, :] = part
            else:
                out_ref[r, :] = part.astype(BF16)

    for lo, hi in ((0, self_step), (self_step + 1, steps)):
        if lo < hi:
            remote(send, recv, fs_sem, fr_sem, lo, hi, 0, me).wait_send()
            remote(back, home, bs_sem, br_sem, lo, hi, 0, me).wait_send()


def solution(mesh):
    n = mesh.shape["ep"]
    offsets = step_offsets()

    def local_layer(tokens, w_gate, expert_ids, keep_second, w_in, w_out):
        token_count, model_dim = tokens.shape[1:]
        expert_count = w_gate.shape[1]
        local_experts, _, hidden_dim = w_in.shape
        capacity = 2 * token_count // expert_count
        rows = local_experts * capacity
        any_space = pl.BlockSpec(memory_space=pltpu.HBM)
        vmem = pltpu.VMEM
        out = pl.pallas_call(
            functools.partial(layer_kernel, n, offsets),
            out_shape=jax.ShapeDtypeStruct((token_count, model_dim), BF16),
            in_specs=[any_space] * 6,
            out_specs=pl.BlockSpec(memory_space=vmem),
            scratch_shapes=[
                vmem((token_count, model_dim), BF16),
                vmem((expert_count, model_dim), BF16),
                vmem((2, token_count), jnp.int32),
                vmem((1, token_count), jnp.int32),
                vmem(w_in.shape, BF16),
                vmem(w_out.shape, BF16),
                vmem((CHUNK * rows, token_count), BF16),
                vmem((n, rows, model_dim), BF16),
                vmem((n, rows, model_dim), BF16),
                vmem((n, rows, model_dim), BF16),
                vmem((n, rows, model_dim), BF16),
                vmem((token_count, 128), F32),
                vmem((token_count, n * rows), BF16),
                vmem((token_count, model_dim), F32),
                pltpu.SemaphoreType.REGULAR,
                pltpu.SemaphoreType.DMA((6,)),
                pltpu.SemaphoreType.DMA((1,)),
                pltpu.SemaphoreType.DMA((n // CHUNK,)),
                pltpu.SemaphoreType.DMA((1,)),
                pltpu.SemaphoreType.DMA((n // CHUNK + 1,)),
            ],
            compiler_params=pltpu.CompilerParams(
                collective_id=0, has_side_effects=True, vmem_limit_bytes=48 * 1024 * 1024),
            name="moe_layer",
        )(*[pltpu.with_memory_space_constraint(x, pltpu.HBM)
            for x in (tokens[0], w_gate.T, expert_ids[0].T, keep_second, w_in, w_out)])
        return out[None]

    group_spec = P(("dp", "ep"))
    return jax.shard_map(
        local_layer, mesh=mesh, in_specs=(group_spec, P(), group_spec, group_spec, P("ep"), P("ep")),
        out_specs=group_spec, check_vma=False)
```

```python
import functools
import math

import jax
import jax.numpy as jnp
from jax import lax
from jax.experimental import pallas as pl
from jax.experimental.pallas import tpu as pltpu
from jax.sharding import PartitionSpec as P

F32 = jnp.float32
BF16 = jnp.bfloat16
MESH = pl.DeviceIdType.MESH
CHUNK = 8


def step_offsets():
    chunks = [
        [(2, 1), (2, -1), (0, 1), (0, -1)],
        [(1, 2), (-1, 2), (1, 0), (-1, 0)],
        [(1, 1), (-1, -1), (1, -1), (-1, 1)],
        [(0, 2), (2, 0), (2, 2)],
    ]
    order = []
    for chunk in chunks:
        order += [(y, x, core) for core in range(2) for (y, x) in chunk]
        if len(chunk) < CHUNK // 2:
            order += [(0, 0, 1), (0, 0, 0)]
    return order


def layer_kernel(
    n, offsets, tok_hbm, wg_hbm, ids_hbm, keep_hbm, wi_hbm, wo_hbm, acc, last_cw, last_home,
    tok, wg, ids, keep, wi, wo, onehot, send, recv, back, home, cols, cw,
    ready_sem, local_sem, fs_sem, fr_sem, bs_sem, br_sem,
):
    side = math.isqrt(n // 2)
    token_count, model_dim = tok.shape
    expert_count = wg.shape[0]
    local_experts, _, hidden_dim = wi.shape
    steps, rows, _ = send.shape
    capacity = rows // local_experts
    chunks = steps // CHUNK
    span = CHUNK * rows
    self_step = offsets.index((0, 0, 0))

    loads = [
        pltpu.make_async_copy(src, dst, local_sem.at[i])
        for i, (src, dst) in enumerate(
            [(ids_hbm, ids), (keep_hbm, keep), (tok_hbm, tok), (wg_hbm, wg), (wi_hbm, wi), (wo_hbm, wo)])
    ]
    for load in loads[:4]:
        load.start()

    me = lax.axis_index("ep")
    my_y, my_x, my_core = me // (2 * side), (me // 2) % side, me % 2

    def peer(step, sign):
        dy, dx, core = offsets[step]
        y, x = (my_y + sign * dy + side) % side, (my_x + sign * dx + side) % side
        return (y * side + x) * 2 + (my_core + core) % 2

    dst = [peer(k, 1) for k in range(steps)]
    src = [peer(k, -1) for k in range(steps)]

    hops = [sum(min(d % side, -d % side) for d in (y, x)) for (y, x, _) in offsets]
    near = sorted((k for k in range(steps) if k != self_step and hops[k] <= 3), key=lambda k: -hops[k])
    first_far = min(k for k in range(steps) if hops[k] > 3) // CHUNK * CHUNK
    barrier = pltpu.get_barrier_semaphore()
    for k in near:
        pl.semaphore_signal(barrier, inc=1, device_id={"ep": dst[k]}, device_id_type=MESH)

    forth_runs = [(c * CHUNK, (c + 1) * CHUNK) for c in range(chunks)]
    home_runs = forth_runs[:-1] + [(steps - CHUNK, steps - CHUNK // 2), (steps - CHUNK // 2, steps)]

    def travel(lo, hi):
        return lo, hi - 1 if hi - 1 == self_step else hi

    def remote(buf_from, buf_to, ssem, rsem, lo, hi, run, device):
        return pltpu.make_async_remote_copy(
            src_ref=buf_from.at[lo:hi], dst_ref=buf_to.at[lo:hi], send_sem=ssem.at[0], recv_sem=rsem.at[run],
            device_id={"ep": device}, device_id_type=MESH)

    def run_of(runs, k):
        return next(i for i, (lo, hi) in enumerate(runs) if lo <= k < hi)

    def start_forth(k):
        remote(send, recv, fs_sem, fr_sem, k, k + 1, run_of(forth_runs, k), dst[k]).start()

    def start_home(k):
        remote(back, home, bs_sem, br_sem, k, k + 1, run_of(home_runs, k), src[k]).start()

    def wait_forth(run):
        remote(send, recv, fs_sem, fr_sem, *travel(*forth_runs[run]), run, me).wait_recv()

    def wait_home(run):
        remote(back, home, bs_sem, br_sem, *travel(*home_runs[run]), run, me).wait_recv()

    loads[0].wait()
    loads[1].wait()
    first_id, second_id = ids[0:1, :], ids[1:2, :]
    used = keep[...] == 1
    expert_row = lax.broadcasted_iota(jnp.int32, (expert_count, token_count), 0)
    first_hot = jnp.where(expert_row == first_id, 1.0, 0.0).astype(F32)
    second_hot = jnp.where((expert_row == second_id) & used, 1.0, 0.0).astype(F32)
    first_total = jnp.sum(first_hot, axis=1, keepdims=True)
    both = jnp.concatenate([first_hot, second_hot], axis=0)
    both16 = both.astype(BF16)
    width = 256
    before = jnp.where(
        lax.broadcasted_iota(jnp.int32, (width, width), 0) < lax.broadcasted_iota(jnp.int32, (width, width), 1),
        1.0, 0.0).astype(BF16)
    carry = jnp.concatenate([jnp.zeros((expert_count, 1), F32), first_total], axis=0)
    pos = []
    for b in range(token_count // width):
        part = both[:, b * width:(b + 1) * width]
        ahead = jnp.dot(both16[:, b * width:(b + 1) * width], before, preferred_element_type=F32) + carry
        picked = part * ahead
        pos.append((jnp.sum(picked[:expert_count], axis=0, keepdims=True), jnp.sum(picked[expert_count:], axis=0, keepdims=True)))
        carry = carry + jnp.sum(part, axis=1, keepdims=True)
    pos_first = jnp.concatenate([p[0] for p in pos], axis=1).astype(jnp.int32)
    pos_second = jnp.concatenate([p[1] for p in pos], axis=1).astype(jnp.int32)
    slot_first = jnp.where(pos_first < capacity, first_id * capacity + pos_first, -1)
    slot_second = jnp.where(used & (pos_second < capacity), second_id * capacity + pos_second, -1)

    loads[2].wait()
    for lo, hi in [(0, CHUNK // 2), (CHUNK // 2, CHUNK)] + [(c * CHUNK, (c + 1) * CHUNK) for c in range(1, chunks)]:
        for k in range(lo, hi):
            slot = dst[k] * rows + lax.broadcasted_iota(jnp.int32, (rows, token_count), 0)
            hit = (slot == slot_first) | (slot == slot_second)
            onehot[(k - lo) * rows:(k - lo + 1) * rows, :] = jnp.where(hit, 1.0, 0.0).astype(BF16)
        for col in range(0, model_dim, width):
            picked = jnp.dot(onehot[:(hi - lo) * rows, :], tok[:, col:col + width], preferred_element_type=F32).astype(BF16)
            for k in range(lo, hi):
                target = recv if k == self_step else send
                target[k, :, col:col + width] = picked[(k - lo) * rows:(k - lo + 1) * rows]
        if lo == 0:
            pl.semaphore_wait(barrier, len(near))
        if lo == first_far:
            pl.semaphore_wait(ready_sem, len(near))
        for k in range(lo, hi):
            if k != self_step:
                start_forth(k)
        if lo == 0:
            for k in near:
                pl.semaphore_signal(ready_sem, inc=1, device_id={"ep": dst[k]}, device_id_type=MESH)
            for load in loads[4:]:
                load.start()

    loads[3].wait()
    logits = lax.dot_general(wg[...], tok[...], (((1,), (1,)), ((), ())), preferred_element_type=F32)
    top = jnp.max(logits, axis=0, keepdims=True)
    raised = jnp.exp(logits - top)
    probs = raised / jnp.sum(raised, axis=0, keepdims=True)
    expert_row = lax.broadcasted_iota(jnp.int32, (expert_count, token_count), 0)
    gate_first = jnp.sum(jnp.where(expert_row == first_id, probs, 0.0), axis=0, keepdims=True)
    gate_second = jnp.sum(jnp.where((expert_row == second_id) & used, probs, 0.0), axis=0, keepdims=True)
    gate_total = gate_first + gate_second
    lines = jnp.concatenate(
        [slot_first.astype(F32), slot_second.astype(F32), gate_first / gate_total, gate_second / gate_total,
         jnp.zeros((124, token_count), F32)], axis=0)
    cols[...] = jnp.transpose(lines)
    block = 64
    for c in range(chunks):
        lane = lax.broadcasted_iota(jnp.int32, (1, span), 1)
        slot = lane % rows
        for j in range(CHUNK):
            slot = slot + jnp.where(lane // rows == j, dst[c * CHUNK + j] * rows, 0)
        slot = slot.astype(F32)

        @pl.loop(0, token_count // block)
        def _(i):
            r = pl.ds(pl.multiple_of(i * block, block), block)
            line = cols[r, :]
            weight = jnp.where(line[:, 0:1] == slot, line[:, 2:3], 0.0) + jnp.where(line[:, 1:2] == slot, line[:, 3:4], 0.0)
            weight = weight.astype(BF16)
            cw[r, c * span:(c + 1) * span] = weight
            if c == chunks - 1:
                last_cw[r, :] = weight[:, span // 2:]

    for load in loads[4:]:
        load.wait()
    for c in range(chunks):
        wait_forth(c)

        @pl.loop(0, local_experts)
        def _(e):
            r = pl.ds(pl.multiple_of(e * capacity, capacity), capacity)
            x = recv[c * CHUNK:(c + 1) * CHUNK, r, :].reshape(CHUNK * capacity, model_dim)
            y = jnp.zeros((CHUNK * capacity, model_dim), F32)
            tile = 768
            for h in range(0, hidden_dim, tile):
                hidden = jnp.dot(x, wi[e, :, h:h + tile], preferred_element_type=F32)
                hidden = jnp.maximum(hidden, 0.0).astype(BF16)
                y = y + jnp.dot(hidden, wo[e, h:h + tile, :], preferred_element_type=F32)
            y = y.astype(BF16).reshape(CHUNK, capacity, model_dim)
            back[c * CHUNK:(c + 1) * CHUNK, r, :] = y
            if self_step // CHUNK == c:
                home[self_step, r, :] = y[self_step % CHUNK]

        for k in range(c * CHUNK, (c + 1) * CHUNK):
            if k != self_step:
                start_home(k)

    block = 256
    for run, (lo, hi) in enumerate(home_runs[:-1]):
        wait_home(run)

        @pl.loop(0, token_count // block)
        def _(i):
            r = pl.ds(pl.multiple_of(i * block, block), block)
            y = home[lo:hi].reshape((hi - lo) * rows, model_dim)
            part = jnp.dot(cw[r, lo * rows:hi * rows], y, preferred_element_type=F32)
            if lo > 0:
                part = acc[r, :] + part
            acc[r, :] = part

    lo, hi = home_runs[-1]
    wait_home(len(home_runs) - 1)
    last_home[...] = home[lo:hi].reshape((hi - lo) * rows, model_dim)
    for lo, hi in ((0, self_step), (self_step + 1, steps)):
        if lo < hi:
            remote(send, recv, fs_sem, fr_sem, lo, hi, 0, me).wait_send()
            remote(back, home, bs_sem, br_sem, lo, hi, 0, me).wait_send()


def finish_kernel(acc, last_cw, last_home, out_hbm, out, sem):
    block = 256
    copies = []
    for i in range(out.shape[0] // block):
        r = pl.ds(i * block, block)
        part = acc[r, :] + jnp.dot(last_cw[r, :], last_home[...], preferred_element_type=F32)
        out[r, :] = part.astype(BF16)
        copies.append(pltpu.make_async_copy(out.at[r], out_hbm.at[r], sem.at[i]))
        copies[-1].start()
    for copy in copies:
        copy.wait()


def solution(mesh):
    n = mesh.shape["ep"]
    offsets = step_offsets()

    def local_layer(tokens, w_gate, expert_ids, keep_second, w_in, w_out):
        token_count, model_dim = tokens.shape[1:]
        expert_count = w_gate.shape[1]
        local_experts, _, hidden_dim = w_in.shape
        capacity = 2 * token_count // expert_count
        rows = local_experts * capacity
        any_space = pl.BlockSpec(memory_space=pltpu.HBM)
        vmem = pltpu.VMEM
        last = CHUNK // 2 * rows
        parts = pl.pallas_call(
            functools.partial(layer_kernel, n, offsets),
            out_shape=[
                jax.ShapeDtypeStruct((token_count, model_dim), F32),
                jax.ShapeDtypeStruct((token_count, last), BF16),
                jax.ShapeDtypeStruct((last, model_dim), BF16),
            ],
            in_specs=[any_space] * 6,
            out_specs=[pl.BlockSpec(memory_space=vmem)] * 3,
            scratch_shapes=[
                vmem((token_count, model_dim), BF16),
                vmem((expert_count, model_dim), BF16),
                vmem((2, token_count), jnp.int32),
                vmem((1, token_count), jnp.int32),
                vmem(w_in.shape, BF16),
                vmem(w_out.shape, BF16),
                vmem((CHUNK * rows, token_count), BF16),
                vmem((n, rows, model_dim), BF16),
                vmem((n, rows, model_dim), BF16),
                vmem((n, rows, model_dim), BF16),
                vmem((n, rows, model_dim), BF16),
                vmem((token_count, 128), F32),
                vmem((token_count, n * rows), BF16),
                pltpu.SemaphoreType.REGULAR,
                pltpu.SemaphoreType.DMA((6,)),
                pltpu.SemaphoreType.DMA((1,)),
                pltpu.SemaphoreType.DMA((n // CHUNK,)),
                pltpu.SemaphoreType.DMA((1,)),
                pltpu.SemaphoreType.DMA((n // CHUNK + 1,)),
            ],
            compiler_params=pltpu.CompilerParams(
                collective_id=0, has_side_effects=True, vmem_limit_bytes=48 * 1024 * 1024),
            name="moe_layer",
        )(*[pltpu.with_memory_space_constraint(x, pltpu.HBM)
            for x in (tokens[0], w_gate.T, expert_ids[0].T, keep_second, w_in, w_out)])
        out = pl.pallas_call(
            finish_kernel,
            out_shape=jax.ShapeDtypeStruct((token_count, model_dim), BF16),
            in_specs=[pl.BlockSpec(memory_space=vmem)] * 3,
            out_specs=pl.BlockSpec(memory_space=pltpu.HBM),
            scratch_shapes=[vmem((token_count, model_dim), BF16), pltpu.SemaphoreType.DMA((token_count // 256,))],
            compiler_params=pltpu.CompilerParams(vmem_limit_bytes=16 * 1024 * 1024),
            name="finish",
        )(*parts)
        return out[None]

    group_spec = P(("dp", "ep"))
    return jax.shard_map(
        local_layer, mesh=mesh, in_specs=(group_spec, P(), group_spec, group_spec, P("ep"), P("ep")),
        out_specs=group_spec, check_vma=False)
```

```python
import functools
import math

import jax
import jax.numpy as jnp
from jax import lax
from jax.experimental import pallas as pl
from jax.experimental.pallas import tpu as pltpu
from jax.sharding import PartitionSpec as P

F32 = jnp.float32
BF16 = jnp.bfloat16
MESH = pl.DeviceIdType.MESH
CHUNK = 8


def step_offsets():
    chunks = [
        [(2, 1), (2, -1), (0, 1), (0, -1)],
        [(1, 2), (-1, 2), (1, 0), (-1, 0)],
        [(0, 2), (2, 0), (2, 2)],
        [(1, 1), (-1, -1), (1, -1), (-1, 1)],
    ]
    order = []
    for chunk in chunks:
        order += [(y, x, core) for core in range(2) for (y, x) in chunk]
        if len(chunk) < CHUNK // 2:
            order += [(0, 0, 1), (0, 0, 0)]
    return order


def layer_kernel(
    n, offsets, tok_hbm, wg_hbm, ids_hbm, keep_hbm, wi_hbm, wo_hbm, acc, last_cw, last_home,
    tok, wg, ids, keep, wi, wo, onehot, send, recv, back, home, cols, cw,
    local_sem, fs_sem, fr_sem, bs_sem, br_sem,
):
    side = math.isqrt(n // 2)
    token_count, model_dim = tok.shape
    expert_count = wg.shape[0]
    local_experts, _, hidden_dim = wi.shape
    steps, rows, _ = send.shape
    capacity = rows // local_experts
    chunks = steps // CHUNK
    span = CHUNK * rows
    self_step = offsets.index((0, 0, 0))

    loads = [
        pltpu.make_async_copy(src, dst, local_sem.at[i])
        for i, (src, dst) in enumerate(
            [(ids_hbm, ids), (keep_hbm, keep), (tok_hbm, tok), (wg_hbm, wg), (wi_hbm, wi), (wo_hbm, wo)])
    ]
    for load in loads[:4]:
        load.start()

    me = lax.axis_index("ep")
    my_y, my_x, my_core = me // (2 * side), (me // 2) % side, me % 2

    def peer(step, sign):
        dy, dx, core = offsets[step]
        y, x = (my_y + sign * dy + side) % side, (my_x + sign * dx + side) % side
        return (y * side + x) * 2 + (my_core + core) % 2

    dst = [peer(k, 1) for k in range(steps)]
    src = [peer(k, -1) for k in range(steps)]

    hop = lambda d: min(d % side, -d % side)
    barrier = pltpu.get_barrier_semaphore()
    peers = [k for k in range(steps) if k != self_step]
    for k in sorted(peers, key=lambda k: -hop(offsets[k][0]) - hop(offsets[k][1])):
        pl.semaphore_signal(barrier, inc=1, device_id={"ep": dst[k]}, device_id_type=MESH)

    forth_runs = [(c * CHUNK, (c + 1) * CHUNK) for c in range(chunks)]
    home_runs = forth_runs[:-1] + [(steps - CHUNK, steps - CHUNK // 2), (steps - CHUNK // 2, steps)]

    def travel(lo, hi):
        return lo, hi - 1 if hi - 1 == self_step else hi

    def remote(buf_from, buf_to, ssem, rsem, lo, hi, run, device):
        return pltpu.make_async_remote_copy(
            src_ref=buf_from.at[lo:hi], dst_ref=buf_to.at[lo:hi], send_sem=ssem.at[0], recv_sem=rsem.at[run],
            device_id={"ep": device}, device_id_type=MESH)

    def run_of(runs, k):
        return next(i for i, (lo, hi) in enumerate(runs) if lo <= k < hi)

    def start_forth(k):
        remote(send, recv, fs_sem, fr_sem, k, k + 1, run_of(forth_runs, k), dst[k]).start()

    def start_home(k):
        remote(back, home, bs_sem, br_sem, k, k + 1, run_of(home_runs, k), src[k]).start()

    def wait_forth(run):
        remote(send, recv, fs_sem, fr_sem, *travel(*forth_runs[run]), run, me).wait_recv()

    def wait_home(run):
        remote(back, home, bs_sem, br_sem, *travel(*home_runs[run]), run, me).wait_recv()

    loads[0].wait()
    loads[1].wait()
    first_id, second_id = ids[0:1, :], ids[1:2, :]
    used = keep[...] == 1
    expert_row = lax.broadcasted_iota(jnp.int32, (expert_count, token_count), 0)
    first_hot = jnp.where(expert_row == first_id, 1.0, 0.0).astype(F32)
    second_hot = jnp.where((expert_row == second_id) & used, 1.0, 0.0).astype(F32)
    first_total = jnp.sum(first_hot, axis=1, keepdims=True)
    both = jnp.concatenate([first_hot, second_hot], axis=0)
    both16 = both.astype(BF16)
    width = 256
    before = jnp.where(
        lax.broadcasted_iota(jnp.int32, (width, width), 0) < lax.broadcasted_iota(jnp.int32, (width, width), 1),
        1.0, 0.0).astype(BF16)
    carry = jnp.concatenate([jnp.zeros((expert_count, 1), F32), first_total], axis=0)
    pos = []
    for b in range(token_count // width):
        part = both[:, b * width:(b + 1) * width]
        ahead = jnp.dot(both16[:, b * width:(b + 1) * width], before, preferred_element_type=F32) + carry
        picked = part * ahead
        pos.append((jnp.sum(picked[:expert_count], axis=0, keepdims=True), jnp.sum(picked[expert_count:], axis=0, keepdims=True)))
        carry = carry + jnp.sum(part, axis=1, keepdims=True)
    pos_first = jnp.concatenate([p[0] for p in pos], axis=1).astype(jnp.int32)
    pos_second = jnp.concatenate([p[1] for p in pos], axis=1).astype(jnp.int32)
    slot_first = jnp.where(pos_first < capacity, first_id * capacity + pos_first, -1)
    slot_second = jnp.where(used & (pos_second < capacity), second_id * capacity + pos_second, -1)

    loads[2].wait()
    for lo, hi in [(0, CHUNK // 2), (CHUNK // 2, CHUNK)] + [(c * CHUNK, (c + 1) * CHUNK) for c in range(1, chunks)]:
        for k in range(lo, hi):
            slot = dst[k] * rows + lax.broadcasted_iota(jnp.int32, (rows, token_count), 0)
            hit = (slot == slot_first) | (slot == slot_second)
            onehot[(k - lo) * rows:(k - lo + 1) * rows, :] = jnp.where(hit, 1.0, 0.0).astype(BF16)
        for col in range(0, model_dim, width):
            picked = jnp.dot(onehot[:(hi - lo) * rows, :], tok[:, col:col + width], preferred_element_type=F32).astype(BF16)
            for k in range(lo, hi):
                target = recv if k == self_step else send
                target[k, :, col:col + width] = picked[(k - lo) * rows:(k - lo + 1) * rows]
        if lo == 0:
            pl.semaphore_wait(barrier, n - 1)
        for k in range(lo, hi):
            if k != self_step:
                start_forth(k)
        if lo == 0:
            for load in loads[4:]:
                load.start()

    loads[3].wait()
    logits = lax.dot_general(wg[...], tok[...], (((1,), (1,)), ((), ())), preferred_element_type=F32)
    top = jnp.max(logits, axis=0, keepdims=True)
    raised = jnp.exp(logits - top)
    probs = raised / jnp.sum(raised, axis=0, keepdims=True)
    expert_row = lax.broadcasted_iota(jnp.int32, (expert_count, token_count), 0)
    gate_first = jnp.sum(jnp.where(expert_row == first_id, probs, 0.0), axis=0, keepdims=True)
    gate_second = jnp.sum(jnp.where((expert_row == second_id) & used, probs, 0.0), axis=0, keepdims=True)
    gate_total = gate_first + gate_second
    lines = jnp.concatenate(
        [slot_first.astype(F32), slot_second.astype(F32), gate_first / gate_total, gate_second / gate_total,
         jnp.zeros((124, token_count), F32)], axis=0)
    cols[...] = jnp.transpose(lines)
    block = 64
    for c in range(chunks):
        lane = lax.broadcasted_iota(jnp.int32, (1, span), 1)
        slot = lane % rows
        for j in range(CHUNK):
            slot = slot + jnp.where(lane // rows == j, dst[c * CHUNK + j] * rows, 0)
        slot = slot.astype(F32)

        @pl.loop(0, token_count // block)
        def _(i):
            r = pl.ds(pl.multiple_of(i * block, block), block)
            line = cols[r, :]
            weight = jnp.where(line[:, 0:1] == slot, line[:, 2:3], 0.0) + jnp.where(line[:, 1:2] == slot, line[:, 3:4], 0.0)
            weight = weight.astype(BF16)
            cw[r, c * span:(c + 1) * span] = weight
            if c == chunks - 1:
                last_cw[r, :] = weight[:, span // 2:]

    for load in loads[4:]:
        load.wait()
    for c in range(chunks):
        wait_forth(c)

        @pl.loop(0, local_experts)
        def _(e):
            r = pl.ds(pl.multiple_of(e * capacity, capacity), capacity)
            x = recv[c * CHUNK:(c + 1) * CHUNK, r, :].reshape(CHUNK * capacity, model_dim)
            y = jnp.zeros((CHUNK * capacity, model_dim), F32)
            tile = 768
            for h in range(0, hidden_dim, tile):
                hidden = jnp.dot(x, wi[e, :, h:h + tile], preferred_element_type=F32)
                hidden = jnp.maximum(hidden, 0.0).astype(BF16)
                y = y + jnp.dot(hidden, wo[e, h:h + tile, :], preferred_element_type=F32)
            y = y.astype(BF16).reshape(CHUNK, capacity, model_dim)
            back[c * CHUNK:(c + 1) * CHUNK, r, :] = y
            if self_step // CHUNK == c:
                home[self_step, r, :] = y[self_step % CHUNK]

        for k in range(c * CHUNK, (c + 1) * CHUNK):
            if k != self_step:
                start_home(k)

    block = 256
    for run, (lo, hi) in enumerate(home_runs[:-1]):
        wait_home(run)

        @pl.loop(0, token_count // block)
        def _(i):
            r = pl.ds(pl.multiple_of(i * block, block), block)
            y = home[lo:hi].reshape((hi - lo) * rows, model_dim)
            part = jnp.dot(cw[r, lo * rows:hi * rows], y, preferred_element_type=F32)
            if lo > 0:
                part = acc[r, :] + part
            acc[r, :] = part

    lo, hi = home_runs[-1]
    wait_home(len(home_runs) - 1)
    last_home[...] = home[lo:hi].reshape((hi - lo) * rows, model_dim)
    for lo, hi in ((0, self_step), (self_step + 1, steps)):
        if lo < hi:
            remote(send, recv, fs_sem, fr_sem, lo, hi, 0, me).wait_send()
            remote(back, home, bs_sem, br_sem, lo, hi, 0, me).wait_send()


def finish_kernel(acc, last_cw, last_home, out_hbm, out, sem):
    block = 256
    copies = []
    for i in range(out.shape[0] // block):
        r = pl.ds(i * block, block)
        part = acc[r, :] + jnp.dot(last_cw[r, :], last_home[...], preferred_element_type=F32)
        out[r, :] = part.astype(BF16)
        copies.append(pltpu.make_async_copy(out.at[r], out_hbm.at[r], sem.at[i]))
        copies[-1].start()
    for copy in copies:
        copy.wait()


def solution(mesh):
    n = mesh.shape["ep"]
    offsets = step_offsets()

    def local_layer(tokens, w_gate, expert_ids, keep_second, w_in, w_out):
        token_count, model_dim = tokens.shape[1:]
        expert_count = w_gate.shape[1]
        local_experts, _, hidden_dim = w_in.shape
        capacity = 2 * token_count // expert_count
        rows = local_experts * capacity
        any_space = pl.BlockSpec(memory_space=pltpu.HBM)
        vmem = pltpu.VMEM
        last = CHUNK // 2 * rows
        parts = pl.pallas_call(
            functools.partial(layer_kernel, n, offsets),
            out_shape=[
                jax.ShapeDtypeStruct((token_count, model_dim), F32),
                jax.ShapeDtypeStruct((token_count, last), BF16),
                jax.ShapeDtypeStruct((last, model_dim), BF16),
            ],
            in_specs=[any_space] * 6,
            out_specs=[pl.BlockSpec(memory_space=vmem)] * 3,
            scratch_shapes=[
                vmem((token_count, model_dim), BF16),
                vmem((expert_count, model_dim), BF16),
                vmem((2, token_count), jnp.int32),
                vmem((1, token_count), jnp.int32),
                vmem(w_in.shape, BF16),
                vmem(w_out.shape, BF16),
                vmem((CHUNK * rows, token_count), BF16),
                vmem((n, rows, model_dim), BF16),
                vmem((n, rows, model_dim), BF16),
                vmem((n, rows, model_dim), BF16),
                vmem((n, rows, model_dim), BF16),
                vmem((token_count, 128), F32),
                vmem((token_count, n * rows), BF16),
                pltpu.SemaphoreType.DMA((6,)),
                pltpu.SemaphoreType.DMA((1,)),
                pltpu.SemaphoreType.DMA((n // CHUNK,)),
                pltpu.SemaphoreType.DMA((1,)),
                pltpu.SemaphoreType.DMA((n // CHUNK + 1,)),
            ],
            compiler_params=pltpu.CompilerParams(
                collective_id=0, has_side_effects=True, vmem_limit_bytes=48 * 1024 * 1024),
            name="moe_layer",
        )(*[pltpu.with_memory_space_constraint(x, pltpu.HBM)
            for x in (tokens[0], w_gate.T, expert_ids[0].T, keep_second, w_in, w_out)])
        out = pl.pallas_call(
            finish_kernel,
            out_shape=jax.ShapeDtypeStruct((token_count, model_dim), BF16),
            in_specs=[pl.BlockSpec(memory_space=vmem)] * 3,
            out_specs=pl.BlockSpec(memory_space=pltpu.HBM),
            scratch_shapes=[vmem((token_count, model_dim), BF16), pltpu.SemaphoreType.DMA((token_count // 256,))],
            compiler_params=pltpu.CompilerParams(vmem_limit_bytes=16 * 1024 * 1024),
            name="finish",
        )(*parts)
        return out[None]

    group_spec = P(("dp", "ep"))
    return jax.shard_map(
        local_layer, mesh=mesh, in_specs=(group_spec, P(), group_spec, group_spec, P("ep"), P("ep")),
        out_specs=group_spec, check_vma=False)
```

```python
import functools
import math

import jax
import jax.numpy as jnp
from jax import lax
from jax.experimental import pallas as pl
from jax.experimental.pallas import tpu as pltpu
from jax.sharding import PartitionSpec as P

F32 = jnp.float32
BF16 = jnp.bfloat16
MESH = pl.DeviceIdType.MESH
CHUNK = 8


def step_offsets():
    chunks = [
        [(2, 1), (2, -1), (0, 1), (0, -1)],
        [(1, 2), (-1, 2), (1, 0), (-1, 0)],
        [(0, 2), (2, 0), (2, 2)],
        [(1, 1), (-1, -1), (1, -1), (-1, 1)],
    ]
    order = []
    for chunk in chunks:
        order += [(y, x, core) for core in range(2) for (y, x) in chunk]
        if len(chunk) < CHUNK // 2:
            order += [(0, 0, 1), (0, 0, 0)]
    return order


def layer_kernel(
    n, offsets, tok_hbm, wg_hbm, ids_hbm, keep_hbm, wi_hbm, wo_hbm, acc, last_cw, last_home,
    tok, wg, ids, keep, wi, wo, onehot, send, recv, back, home, cols, cw,
    ready_sem, local_sem, fs_sem, fr_sem, bs_sem, br_sem,
):
    side = math.isqrt(n // 2)
    token_count, model_dim = tok.shape
    expert_count = wg.shape[0]
    local_experts, _, hidden_dim = wi.shape
    steps, rows, _ = send.shape
    capacity = rows // local_experts
    chunks = steps // CHUNK
    span = CHUNK * rows
    self_step = offsets.index((0, 0, 0))

    loads = [
        pltpu.make_async_copy(src, dst, local_sem.at[i])
        for i, (src, dst) in enumerate(
            [(ids_hbm, ids), (keep_hbm, keep), (tok_hbm, tok), (wg_hbm, wg), (wi_hbm, wi), (wo_hbm, wo)])
    ]
    for load in loads[:4]:
        load.start()

    me = lax.axis_index("ep")
    my_y, my_x, my_core = me // (2 * side), (me // 2) % side, me % 2

    def peer(step, sign):
        dy, dx, core = offsets[step]
        y, x = (my_y + sign * dy + side) % side, (my_x + sign * dx + side) % side
        return (y * side + x) * 2 + (my_core + core) % 2

    dst = [peer(k, 1) for k in range(steps)]
    src = [peer(k, -1) for k in range(steps)]

    hops = [sum(min(d % side, -d % side) for d in (y, x)) for (y, x, _) in offsets]
    near = sorted((k for k in range(steps) if k != self_step and hops[k] <= 3), key=lambda k: -hops[k])
    first_far = min(k for k in range(steps) if hops[k] > 3) // CHUNK * CHUNK
    barrier = pltpu.get_barrier_semaphore()
    for k in near:
        pl.semaphore_signal(barrier, inc=1, device_id={"ep": dst[k]}, device_id_type=MESH)

    forth_runs = [(c * CHUNK, (c + 1) * CHUNK) for c in range(chunks)]
    home_runs = forth_runs[:-1] + [(steps - CHUNK, steps - CHUNK // 2), (steps - CHUNK // 2, steps)]

    def travel(lo, hi):
        return lo, hi - 1 if hi - 1 == self_step else hi

    def remote(buf_from, buf_to, ssem, rsem, lo, hi, run, device):
        return pltpu.make_async_remote_copy(
            src_ref=buf_from.at[lo:hi], dst_ref=buf_to.at[lo:hi], send_sem=ssem.at[0], recv_sem=rsem.at[run],
            device_id={"ep": device}, device_id_type=MESH)

    def run_of(runs, k):
        return next(i for i, (lo, hi) in enumerate(runs) if lo <= k < hi)

    def start_forth(k):
        remote(send, recv, fs_sem, fr_sem, k, k + 1, run_of(forth_runs, k), dst[k]).start()

    def start_home(k):
        remote(back, home, bs_sem, br_sem, k, k + 1, run_of(home_runs, k), src[k]).start()

    def wait_forth(run):
        remote(send, recv, fs_sem, fr_sem, *travel(*forth_runs[run]), run, me).wait_recv()

    def wait_home(run):
        remote(back, home, bs_sem, br_sem, *travel(*home_runs[run]), run, me).wait_recv()

    loads[0].wait()
    loads[1].wait()
    first_id, second_id = ids[0:1, :], ids[1:2, :]
    used = keep[...] == 1
    expert_row = lax.broadcasted_iota(jnp.int32, (expert_count, token_count), 0)
    first_hot = jnp.where(expert_row == first_id, 1.0, 0.0).astype(F32)
    second_hot = jnp.where((expert_row == second_id) & used, 1.0, 0.0).astype(F32)
    first_total = jnp.sum(first_hot, axis=1, keepdims=True)
    both = jnp.concatenate([first_hot, second_hot], axis=0)
    both16 = both.astype(BF16)
    width = 256
    before = jnp.where(
        lax.broadcasted_iota(jnp.int32, (width, width), 0) < lax.broadcasted_iota(jnp.int32, (width, width), 1),
        1.0, 0.0).astype(BF16)
    carry = jnp.concatenate([jnp.zeros((expert_count, 1), F32), first_total], axis=0)
    pos = []
    for b in range(token_count // width):
        part = both[:, b * width:(b + 1) * width]
        ahead = jnp.dot(both16[:, b * width:(b + 1) * width], before, preferred_element_type=F32) + carry
        picked = part * ahead
        pos.append((jnp.sum(picked[:expert_count], axis=0, keepdims=True), jnp.sum(picked[expert_count:], axis=0, keepdims=True)))
        carry = carry + jnp.sum(part, axis=1, keepdims=True)
    pos_first = jnp.concatenate([p[0] for p in pos], axis=1).astype(jnp.int32)
    pos_second = jnp.concatenate([p[1] for p in pos], axis=1).astype(jnp.int32)
    slot_first = jnp.where(pos_first < capacity, first_id * capacity + pos_first, -1)
    slot_second = jnp.where(used & (pos_second < capacity), second_id * capacity + pos_second, -1)

    loads[2].wait()
    for lo, hi in [(0, CHUNK // 2), (CHUNK // 2, CHUNK)] + [(c * CHUNK, (c + 1) * CHUNK) for c in range(1, chunks)]:
        for k in range(lo, hi):
            slot = dst[k] * rows + lax.broadcasted_iota(jnp.int32, (rows, token_count), 0)
            hit = (slot == slot_first) | (slot == slot_second)
            onehot[(k - lo) * rows:(k - lo + 1) * rows, :] = jnp.where(hit, 1.0, 0.0).astype(BF16)
        for col in range(0, model_dim, width):
            picked = jnp.dot(onehot[:(hi - lo) * rows, :], tok[:, col:col + width], preferred_element_type=F32).astype(BF16)
            for k in range(lo, hi):
                target = recv if k == self_step else send
                target[k, :, col:col + width] = picked[(k - lo) * rows:(k - lo + 1) * rows]
        if lo == 0:
            pl.semaphore_wait(barrier, len(near))
        if lo == first_far:
            pl.semaphore_wait(ready_sem, len(near))
        for k in range(lo, hi):
            if k != self_step:
                start_forth(k)
        if lo == CHUNK // 2:
            for k in near:
                pl.semaphore_signal(ready_sem, inc=1, device_id={"ep": dst[k]}, device_id_type=MESH)
        if lo == 0:
            for load in loads[4:]:
                load.start()

    loads[3].wait()
    logits = lax.dot_general(wg[...], tok[...], (((1,), (1,)), ((), ())), preferred_element_type=F32)
    top = jnp.max(logits, axis=0, keepdims=True)
    raised = jnp.exp(logits - top)
    probs = raised / jnp.sum(raised, axis=0, keepdims=True)
    expert_row = lax.broadcasted_iota(jnp.int32, (expert_count, token_count), 0)
    gate_first = jnp.sum(jnp.where(expert_row == first_id, probs, 0.0), axis=0, keepdims=True)
    gate_second = jnp.sum(jnp.where((expert_row == second_id) & used, probs, 0.0), axis=0, keepdims=True)
    gate_total = gate_first + gate_second
    lines = jnp.concatenate(
        [slot_first.astype(F32), slot_second.astype(F32), gate_first / gate_total, gate_second / gate_total,
         jnp.zeros((124, token_count), F32)], axis=0)
    cols[...] = jnp.transpose(lines)
    block = 64
    for c in range(chunks):
        lane = lax.broadcasted_iota(jnp.int32, (1, span), 1)
        slot = lane % rows
        for j in range(CHUNK):
            slot = slot + jnp.where(lane // rows == j, dst[c * CHUNK + j] * rows, 0)
        slot = slot.astype(F32)

        @pl.loop(0, token_count // block)
        def _(i):
            r = pl.ds(pl.multiple_of(i * block, block), block)
            line = cols[r, :]
            weight = jnp.where(line[:, 0:1] == slot, line[:, 2:3], 0.0) + jnp.where(line[:, 1:2] == slot, line[:, 3:4], 0.0)
            weight = weight.astype(BF16)
            cw[r, c * span:(c + 1) * span] = weight
            if c == chunks - 1:
                last_cw[r, :] = weight[:, span // 2:]

    for load in loads[4:]:
        load.wait()
    for c in range(chunks):
        wait_forth(c)

        @pl.loop(0, local_experts)
        def _(e):
            r = pl.ds(pl.multiple_of(e * capacity, capacity), capacity)
            x = recv[c * CHUNK:(c + 1) * CHUNK, r, :].reshape(CHUNK * capacity, model_dim)
            y = jnp.zeros((CHUNK * capacity, model_dim), F32)
            tile = 768
            for h in range(0, hidden_dim, tile):
                hidden = jnp.dot(x, wi[e, :, h:h + tile], preferred_element_type=F32)
                hidden = jnp.maximum(hidden, 0.0).astype(BF16)
                y = y + jnp.dot(hidden, wo[e, h:h + tile, :], preferred_element_type=F32)
            y = y.astype(BF16).reshape(CHUNK, capacity, model_dim)
            back[c * CHUNK:(c + 1) * CHUNK, r, :] = y
            if self_step // CHUNK == c:
                home[self_step, r, :] = y[self_step % CHUNK]

        for k in range(c * CHUNK, (c + 1) * CHUNK):
            if k != self_step:
                start_home(k)

    block = 256
    for run, (lo, hi) in enumerate(home_runs[:-1]):
        wait_home(run)

        @pl.loop(0, token_count // block)
        def _(i):
            r = pl.ds(pl.multiple_of(i * block, block), block)
            y = home[lo:hi].reshape((hi - lo) * rows, model_dim)
            part = jnp.dot(cw[r, lo * rows:hi * rows], y, preferred_element_type=F32)
            if lo > 0:
                part = acc[r, :] + part
            acc[r, :] = part

    lo, hi = home_runs[-1]
    wait_home(len(home_runs) - 1)
    last_home[...] = home[lo:hi].reshape((hi - lo) * rows, model_dim)
    for lo, hi in ((0, self_step), (self_step + 1, steps)):
        if lo < hi:
            remote(send, recv, fs_sem, fr_sem, lo, hi, 0, me).wait_send()
            remote(back, home, bs_sem, br_sem, lo, hi, 0, me).wait_send()


def finish_kernel(acc, last_cw, last_home, out_hbm, out, sem):
    block = 256
    copies = []
    for i in range(out.shape[0] // block):
        r = pl.ds(i * block, block)
        part = acc[r, :] + jnp.dot(last_cw[r, :], last_home[...], preferred_element_type=F32)
        out[r, :] = part.astype(BF16)
        copies.append(pltpu.make_async_copy(out.at[r], out_hbm.at[r], sem.at[i]))
        copies[-1].start()
    for copy in copies:
        copy.wait()


def solution(mesh):
    n = mesh.shape["ep"]
    offsets = step_offsets()

    def local_layer(tokens, w_gate, expert_ids, keep_second, w_in, w_out):
        token_count, model_dim = tokens.shape[1:]
        expert_count = w_gate.shape[1]
        local_experts, _, hidden_dim = w_in.shape
        capacity = 2 * token_count // expert_count
        rows = local_experts * capacity
        any_space = pl.BlockSpec(memory_space=pltpu.HBM)
        vmem = pltpu.VMEM
        last = CHUNK // 2 * rows
        parts = pl.pallas_call(
            functools.partial(layer_kernel, n, offsets),
            out_shape=[
                jax.ShapeDtypeStruct((token_count, model_dim), F32),
                jax.ShapeDtypeStruct((token_count, last), BF16),
                jax.ShapeDtypeStruct((last, model_dim), BF16),
            ],
            in_specs=[any_space] * 6,
            out_specs=[pl.BlockSpec(memory_space=vmem)] * 3,
            scratch_shapes=[
                vmem((token_count, model_dim), BF16),
                vmem((expert_count, model_dim), BF16),
                vmem((2, token_count), jnp.int32),
                vmem((1, token_count), jnp.int32),
                vmem(w_in.shape, BF16),
                vmem(w_out.shape, BF16),
                vmem((CHUNK * rows, token_count), BF16),
                vmem((n, rows, model_dim), BF16),
                vmem((n, rows, model_dim), BF16),
                vmem((n, rows, model_dim), BF16),
                vmem((n, rows, model_dim), BF16),
                vmem((token_count, 128), F32),
                vmem((token_count, n * rows), BF16),
                pltpu.SemaphoreType.REGULAR,
                pltpu.SemaphoreType.DMA((6,)),
                pltpu.SemaphoreType.DMA((1,)),
                pltpu.SemaphoreType.DMA((n // CHUNK,)),
                pltpu.SemaphoreType.DMA((1,)),
                pltpu.SemaphoreType.DMA((n // CHUNK + 1,)),
            ],
            compiler_params=pltpu.CompilerParams(
                collective_id=0, has_side_effects=True, vmem_limit_bytes=48 * 1024 * 1024),
            name="moe_layer",
        )(*[pltpu.with_memory_space_constraint(x, pltpu.HBM)
            for x in (tokens[0], w_gate.T, expert_ids[0].T, keep_second, w_in, w_out)])
        out = pl.pallas_call(
            finish_kernel,
            out_shape=jax.ShapeDtypeStruct((token_count, model_dim), BF16),
            in_specs=[pl.BlockSpec(memory_space=vmem)] * 3,
            out_specs=pl.BlockSpec(memory_space=pltpu.HBM),
            scratch_shapes=[vmem((token_count, model_dim), BF16), pltpu.SemaphoreType.DMA((token_count // 256,))],
            compiler_params=pltpu.CompilerParams(vmem_limit_bytes=16 * 1024 * 1024),
            name="finish",
        )(*parts)
        return out[None]

    group_spec = P(("dp", "ep"))
    return jax.shard_map(
        local_layer, mesh=mesh, in_specs=(group_spec, P(), group_spec, group_spec, P("ep"), P("ep")),
        out_specs=group_spec, check_vma=False)
```

```python
import functools
import math

import jax
import jax.numpy as jnp
from jax import lax
from jax.experimental import pallas as pl
from jax.experimental.pallas import tpu as pltpu
from jax.sharding import PartitionSpec as P

F32 = jnp.float32
BF16 = jnp.bfloat16
MESH = pl.DeviceIdType.MESH
CHUNK = 8


def step_offsets():
    chunks = [
        [(2, 1), (2, -1), (0, 1), (0, -1)],
        [(1, 2), (-1, 2), (1, 0), (-1, 0)],
        [(0, 2), (2, 0), (2, 2)],
        [(1, 1), (-1, -1), (1, -1), (-1, 1)],
    ]
    order = []
    for chunk in chunks:
        order += [(y, x, core) for core in range(2) for (y, x) in chunk]
        if len(chunk) < CHUNK // 2:
            order += [(0, 0, 1), (0, 0, 0)]
    return order


def layer_kernel(
    n, offsets, tok_hbm, wg_hbm, ids_hbm, keep_hbm, wi_hbm, wo_hbm, acc, last_cw, last_home,
    tok, wg, ids, keep, wi, wo, onehot, send, recv, back, home, cols, cw,
    ready_sem, local_sem, fs_sem, fr_sem, bs_sem, br_sem,
):
    side = math.isqrt(n // 2)
    token_count, model_dim = tok.shape
    expert_count = wg.shape[0]
    local_experts, _, hidden_dim = wi.shape
    steps, rows, _ = send.shape
    capacity = rows // local_experts
    chunks = steps // CHUNK
    span = CHUNK * rows
    self_step = offsets.index((0, 0, 0))

    loads = [
        pltpu.make_async_copy(src, dst, local_sem.at[i])
        for i, (src, dst) in enumerate(
            [(ids_hbm, ids), (keep_hbm, keep), (tok_hbm, tok), (wg_hbm, wg), (wi_hbm, wi), (wo_hbm, wo)])
    ]
    for load in loads[:4]:
        load.start()

    me = lax.axis_index("ep")
    my_y, my_x, my_core = me // (2 * side), (me // 2) % side, me % 2

    def peer(step, sign):
        dy, dx, core = offsets[step]
        y, x = (my_y + sign * dy + side) % side, (my_x + sign * dx + side) % side
        return (y * side + x) * 2 + (my_core + core) % 2

    dst = [peer(k, 1) for k in range(steps)]
    src = [peer(k, -1) for k in range(steps)]

    hops = [sum(min(d % side, -d % side) for d in (y, x)) for (y, x, _) in offsets]
    near = sorted((k for k in range(steps) if k != self_step and hops[k] <= 3), key=lambda k: -hops[k])
    first_far = min(k for k in range(steps) if hops[k] > 3) // CHUNK * CHUNK
    halfway = offsets.index((0, side // 2, 0))
    barrier = pltpu.get_barrier_semaphore()
    for k in near:
        pl.semaphore_signal(barrier, inc=1, device_id={"ep": dst[k]}, device_id_type=MESH)

    forth_runs = [(c * CHUNK, (c + 1) * CHUNK) for c in range(chunks)]
    home_runs = forth_runs[:-1] + [(steps - CHUNK, steps - CHUNK // 2), (steps - CHUNK // 2, steps)]

    def travel(lo, hi):
        return lo, hi - 1 if hi - 1 == self_step else hi

    def remote(buf_from, buf_to, ssem, rsem, lo, hi, run, device):
        return pltpu.make_async_remote_copy(
            src_ref=buf_from.at[lo:hi], dst_ref=buf_to.at[lo:hi], send_sem=ssem.at[0], recv_sem=rsem.at[run],
            device_id={"ep": device}, device_id_type=MESH)

    def run_of(runs, k):
        return next(i for i, (lo, hi) in enumerate(runs) if lo <= k < hi)

    def start_forth(k):
        remote(send, recv, fs_sem, fr_sem, k, k + 1, run_of(forth_runs, k), dst[k]).start()

    def start_home(k):
        remote(back, home, bs_sem, br_sem, k, k + 1, run_of(home_runs, k), src[k]).start()

    def wait_forth(run):
        remote(send, recv, fs_sem, fr_sem, *travel(*forth_runs[run]), run, me).wait_recv()

    def wait_home(run):
        remote(back, home, bs_sem, br_sem, *travel(*home_runs[run]), run, me).wait_recv()

    loads[0].wait()
    loads[1].wait()
    first_id, second_id = ids[0:1, :], ids[1:2, :]
    used = keep[...] == 1
    expert_row = lax.broadcasted_iota(jnp.int32, (expert_count, token_count), 0)
    first_hot = jnp.where(expert_row == first_id, 1.0, 0.0).astype(F32)
    second_hot = jnp.where((expert_row == second_id) & used, 1.0, 0.0).astype(F32)
    first_total = jnp.sum(first_hot, axis=1, keepdims=True)
    both = jnp.concatenate([first_hot, second_hot], axis=0)
    both16 = both.astype(BF16)
    width = 256
    before = jnp.where(
        lax.broadcasted_iota(jnp.int32, (width, width), 0) < lax.broadcasted_iota(jnp.int32, (width, width), 1),
        1.0, 0.0).astype(BF16)
    carry = jnp.concatenate([jnp.zeros((expert_count, 1), F32), first_total], axis=0)
    pos = []
    for b in range(token_count // width):
        part = both[:, b * width:(b + 1) * width]
        ahead = jnp.dot(both16[:, b * width:(b + 1) * width], before, preferred_element_type=F32) + carry
        picked = part * ahead
        pos.append((jnp.sum(picked[:expert_count], axis=0, keepdims=True), jnp.sum(picked[expert_count:], axis=0, keepdims=True)))
        carry = carry + jnp.sum(part, axis=1, keepdims=True)
    pos_first = jnp.concatenate([p[0] for p in pos], axis=1).astype(jnp.int32)
    pos_second = jnp.concatenate([p[1] for p in pos], axis=1).astype(jnp.int32)
    slot_first = jnp.where(pos_first < capacity, first_id * capacity + pos_first, -1)
    slot_second = jnp.where(used & (pos_second < capacity), second_id * capacity + pos_second, -1)

    loads[2].wait()
    for lo, hi in [(0, CHUNK // 2), (CHUNK // 2, CHUNK)] + [(c * CHUNK, (c + 1) * CHUNK) for c in range(1, chunks)]:
        for k in range(lo, hi):
            slot = dst[k] * rows + lax.broadcasted_iota(jnp.int32, (rows, token_count), 0)
            hit = (slot == slot_first) | (slot == slot_second)
            onehot[(k - lo) * rows:(k - lo + 1) * rows, :] = jnp.where(hit, 1.0, 0.0).astype(BF16)
        for col in range(0, model_dim, width):
            picked = jnp.dot(onehot[:(hi - lo) * rows, :], tok[:, col:col + width], preferred_element_type=F32).astype(BF16)
            for k in range(lo, hi):
                target = recv if k == self_step else send
                target[k, :, col:col + width] = picked[(k - lo) * rows:(k - lo + 1) * rows]
        if lo == 0:
            pl.semaphore_wait(barrier, len(near))
        if lo == first_far:
            pl.semaphore_wait(ready_sem, 1)
        for k in range(lo, hi):
            if k != self_step:
                start_forth(k)
        if lo == CHUNK // 2:
            pl.semaphore_signal(ready_sem, inc=1, device_id={"ep": dst[halfway]}, device_id_type=MESH)
        if lo == 0:
            for load in loads[4:]:
                load.start()

    loads[3].wait()
    logits = lax.dot_general(wg[...], tok[...], (((1,), (1,)), ((), ())), preferred_element_type=F32)
    top = jnp.max(logits, axis=0, keepdims=True)
    raised = jnp.exp(logits - top)
    probs = raised / jnp.sum(raised, axis=0, keepdims=True)
    expert_row = lax.broadcasted_iota(jnp.int32, (expert_count, token_count), 0)
    gate_first = jnp.sum(jnp.where(expert_row == first_id, probs, 0.0), axis=0, keepdims=True)
    gate_second = jnp.sum(jnp.where((expert_row == second_id) & used, probs, 0.0), axis=0, keepdims=True)
    gate_total = gate_first + gate_second
    lines = jnp.concatenate(
        [slot_first.astype(F32), slot_second.astype(F32), gate_first / gate_total, gate_second / gate_total,
         jnp.zeros((124, token_count), F32)], axis=0)
    cols[...] = jnp.transpose(lines)
    block = 64
    for c in range(chunks):
        lane = lax.broadcasted_iota(jnp.int32, (1, span), 1)
        slot = lane % rows
        for j in range(CHUNK):
            slot = slot + jnp.where(lane // rows == j, dst[c * CHUNK + j] * rows, 0)
        slot = slot.astype(F32)

        @pl.loop(0, token_count // block)
        def _(i):
            r = pl.ds(pl.multiple_of(i * block, block), block)
            line = cols[r, :]
            weight = jnp.where(line[:, 0:1] == slot, line[:, 2:3], 0.0) + jnp.where(line[:, 1:2] == slot, line[:, 3:4], 0.0)
            weight = weight.astype(BF16)
            cw[r, c * span:(c + 1) * span] = weight
            if c == chunks - 1:
                last_cw[r, :] = weight[:, span // 2:]

    for load in loads[4:]:
        load.wait()
    for c in range(chunks):
        wait_forth(c)

        @pl.loop(0, local_experts)
        def _(e):
            r = pl.ds(pl.multiple_of(e * capacity, capacity), capacity)
            x = recv[c * CHUNK:(c + 1) * CHUNK, r, :].reshape(CHUNK * capacity, model_dim)
            y = jnp.zeros((CHUNK * capacity, model_dim), F32)
            tile = 768
            for h in range(0, hidden_dim, tile):
                hidden = jnp.dot(x, wi[e, :, h:h + tile], preferred_element_type=F32)
                hidden = jnp.maximum(hidden, 0.0).astype(BF16)
                y = y + jnp.dot(hidden, wo[e, h:h + tile, :], preferred_element_type=F32)
            y = y.astype(BF16).reshape(CHUNK, capacity, model_dim)
            back[c * CHUNK:(c + 1) * CHUNK, r, :] = y
            if self_step // CHUNK == c:
                home[self_step, r, :] = y[self_step % CHUNK]

        for k in range(c * CHUNK, (c + 1) * CHUNK):
            if k != self_step:
                start_home(k)

    block = 256
    for run, (lo, hi) in enumerate(home_runs[:-1]):
        wait_home(run)

        @pl.loop(0, token_count // block)
        def _(i):
            r = pl.ds(pl.multiple_of(i * block, block), block)
            y = home[lo:hi].reshape((hi - lo) * rows, model_dim)
            part = jnp.dot(cw[r, lo * rows:hi * rows], y, preferred_element_type=F32)
            if lo > 0:
                part = acc[r, :] + part
            acc[r, :] = part

    lo, hi = home_runs[-1]
    wait_home(len(home_runs) - 1)
    last_home[...] = home[lo:hi].reshape((hi - lo) * rows, model_dim)
    for lo, hi in ((0, self_step), (self_step + 1, steps)):
        if lo < hi:
            remote(send, recv, fs_sem, fr_sem, lo, hi, 0, me).wait_send()
            remote(back, home, bs_sem, br_sem, lo, hi, 0, me).wait_send()


def finish_kernel(acc, last_cw, last_home, out_hbm, out, sem):
    block = 256
    copies = []
    for i in range(out.shape[0] // block):
        r = pl.ds(i * block, block)
        part = acc[r, :] + jnp.dot(last_cw[r, :], last_home[...], preferred_element_type=F32)
        out[r, :] = part.astype(BF16)
        copies.append(pltpu.make_async_copy(out.at[r], out_hbm.at[r], sem.at[i]))
        copies[-1].start()
    for copy in copies:
        copy.wait()


def solution(mesh):
    n = mesh.shape["ep"]
    offsets = step_offsets()

    def local_layer(tokens, w_gate, expert_ids, keep_second, w_in, w_out):
        token_count, model_dim = tokens.shape[1:]
        expert_count = w_gate.shape[1]
        local_experts, _, hidden_dim = w_in.shape
        capacity = 2 * token_count // expert_count
        rows = local_experts * capacity
        any_space = pl.BlockSpec(memory_space=pltpu.HBM)
        vmem = pltpu.VMEM
        last = CHUNK // 2 * rows
        parts = pl.pallas_call(
            functools.partial(layer_kernel, n, offsets),
            out_shape=[
                jax.ShapeDtypeStruct((token_count, model_dim), F32),
                jax.ShapeDtypeStruct((token_count, last), BF16),
                jax.ShapeDtypeStruct((last, model_dim), BF16),
            ],
            in_specs=[any_space] * 6,
            out_specs=[pl.BlockSpec(memory_space=vmem)] * 3,
            scratch_shapes=[
                vmem((token_count, model_dim), BF16),
                vmem((expert_count, model_dim), BF16),
                vmem((2, token_count), jnp.int32),
                vmem((1, token_count), jnp.int32),
                vmem(w_in.shape, BF16),
                vmem(w_out.shape, BF16),
                vmem((CHUNK * rows, token_count), BF16),
                vmem((n, rows, model_dim), BF16),
                vmem((n, rows, model_dim), BF16),
                vmem((n, rows, model_dim), BF16),
                vmem((n, rows, model_dim), BF16),
                vmem((token_count, 128), F32),
                vmem((token_count, n * rows), BF16),
                pltpu.SemaphoreType.REGULAR,
                pltpu.SemaphoreType.DMA((6,)),
                pltpu.SemaphoreType.DMA((1,)),
                pltpu.SemaphoreType.DMA((n // CHUNK,)),
                pltpu.SemaphoreType.DMA((1,)),
                pltpu.SemaphoreType.DMA((n // CHUNK + 1,)),
            ],
            compiler_params=pltpu.CompilerParams(
                collective_id=0, has_side_effects=True, vmem_limit_bytes=48 * 1024 * 1024),
            name="moe_layer",
        )(*[pltpu.with_memory_space_constraint(x, pltpu.HBM)
            for x in (tokens[0], w_gate.T, expert_ids[0].T, keep_second, w_in, w_out)])
        out = pl.pallas_call(
            finish_kernel,
            out_shape=jax.ShapeDtypeStruct((token_count, model_dim), BF16),
            in_specs=[pl.BlockSpec(memory_space=vmem)] * 3,
            out_specs=pl.BlockSpec(memory_space=pltpu.HBM),
            scratch_shapes=[vmem((token_count, model_dim), BF16), pltpu.SemaphoreType.DMA((token_count // 256,))],
            compiler_params=pltpu.CompilerParams(vmem_limit_bytes=16 * 1024 * 1024),
            name="finish",
        )(*parts)
        return out[None]

    group_spec = P(("dp", "ep"))
    return jax.shard_map(
        local_layer, mesh=mesh, in_specs=(group_spec, P(), group_spec, group_spec, P("ep"), P("ep")),
        out_specs=group_spec, check_vma=False)
```

```python
import functools
import math

import jax
import jax.numpy as jnp
from jax import lax
from jax.experimental import pallas as pl
from jax.experimental.pallas import tpu as pltpu
from jax.sharding import PartitionSpec as P

F32 = jnp.float32
BF16 = jnp.bfloat16
MESH = pl.DeviceIdType.MESH
CHUNK = 8


def step_offsets():
    chunks = [
        [(2, 1), (2, -1), (0, 1), (0, -1)],
        [(1, 2), (-1, 2), (1, 0), (-1, 0)],
        [(0, 2), (2, 0), (2, 2)],
        [(1, 1), (-1, -1), (1, -1), (-1, 1)],
    ]
    order = []
    for chunk in chunks:
        order += [(y, x, core) for core in range(2) for (y, x) in chunk]
        if len(chunk) < CHUNK // 2:
            order += [(0, 0, 1), (0, 0, 0)]
    return order


def layer_kernel(
    n, offsets, tok_hbm, wg_hbm, ids_hbm, keep_hbm, wi_hbm, wo_hbm, acc, last_cw, last_home,
    tok, wg, ids, keep, wi, wo, onehot, send, recv, back, home, cols, cw,
    ready_sem, local_sem, fs_sem, fr_sem, bs_sem, br_sem,
):
    side = math.isqrt(n // 2)
    token_count, model_dim = tok.shape
    expert_count = wg.shape[0]
    local_experts, _, hidden_dim = wi.shape
    steps, rows, _ = send.shape
    capacity = rows // local_experts
    chunks = steps // CHUNK
    span = CHUNK * rows
    self_step = offsets.index((0, 0, 0))

    loads = [
        pltpu.make_async_copy(src, dst, local_sem.at[i])
        for i, (src, dst) in enumerate(
            [(ids_hbm, ids), (keep_hbm, keep), (tok_hbm, tok), (wg_hbm, wg), (wi_hbm, wi), (wo_hbm, wo)])
    ]
    for load in loads[:4]:
        load.start()

    me = lax.axis_index("ep")
    my_y, my_x, my_core = me // (2 * side), (me // 2) % side, me % 2

    def peer(step, sign):
        dy, dx, core = offsets[step]
        y, x = (my_y + sign * dy + side) % side, (my_x + sign * dx + side) % side
        return (y * side + x) * 2 + (my_core + core) % 2

    dst = [peer(k, 1) for k in range(steps)]
    src = [peer(k, -1) for k in range(steps)]

    hops = [sum(min(d % side, -d % side) for d in (y, x)) for (y, x, _) in offsets]
    near = sorted((k for k in range(steps) if k != self_step and hops[k] <= 3), key=lambda k: -hops[k])
    first_far = min(k for k in range(steps) if hops[k] > 3) // CHUNK * CHUNK
    barrier = pltpu.get_barrier_semaphore()
    for k in near:
        pl.semaphore_signal(barrier, inc=1, device_id={"ep": dst[k]}, device_id_type=MESH)

    forth_runs = [(c * CHUNK, (c + 1) * CHUNK) for c in range(chunks)]
    home_runs = forth_runs[:-1] + [(steps - CHUNK, steps - CHUNK // 2), (steps - CHUNK // 2, steps)]

    def travel(lo, hi):
        return lo, hi - 1 if hi - 1 == self_step else hi

    def remote(buf_from, buf_to, ssem, rsem, lo, hi, run, device):
        return pltpu.make_async_remote_copy(
            src_ref=buf_from.at[lo:hi], dst_ref=buf_to.at[lo:hi], send_sem=ssem.at[0], recv_sem=rsem.at[run],
            device_id={"ep": device}, device_id_type=MESH)

    def run_of(runs, k):
        return next(i for i, (lo, hi) in enumerate(runs) if lo <= k < hi)

    def start_forth(k):
        remote(send, recv, fs_sem, fr_sem, k, k + 1, run_of(forth_runs, k), dst[k]).start()

    def start_home(k):
        remote(back, home, bs_sem, br_sem, k, k + 1, run_of(home_runs, k), src[k]).start()

    def wait_forth(run):
        remote(send, recv, fs_sem, fr_sem, *travel(*forth_runs[run]), run, me).wait_recv()

    def wait_home(run):
        remote(back, home, bs_sem, br_sem, *travel(*home_runs[run]), run, me).wait_recv()

    loads[0].wait()
    loads[1].wait()
    first_id, second_id = ids[0:1, :], ids[1:2, :]
    used = keep[...] == 1
    expert_row = lax.broadcasted_iota(jnp.int32, (expert_count, token_count), 0)
    first_hot = jnp.where(expert_row == first_id, 1.0, 0.0).astype(F32)
    second_hot = jnp.where((expert_row == second_id) & used, 1.0, 0.0).astype(F32)
    first_total = jnp.sum(first_hot, axis=1, keepdims=True)
    both = jnp.concatenate([first_hot, second_hot], axis=0)
    both16 = both.astype(BF16)
    width = 256
    before = jnp.where(
        lax.broadcasted_iota(jnp.int32, (width, width), 0) < lax.broadcasted_iota(jnp.int32, (width, width), 1),
        1.0, 0.0).astype(BF16)
    carry = jnp.concatenate([jnp.zeros((expert_count, 1), F32), first_total], axis=0)
    pos = []
    for b in range(token_count // width):
        part = both[:, b * width:(b + 1) * width]
        ahead = jnp.dot(both16[:, b * width:(b + 1) * width], before, preferred_element_type=F32) + carry
        picked = part * ahead
        pos.append((jnp.sum(picked[:expert_count], axis=0, keepdims=True), jnp.sum(picked[expert_count:], axis=0, keepdims=True)))
        carry = carry + jnp.sum(part, axis=1, keepdims=True)
    pos_first = jnp.concatenate([p[0] for p in pos], axis=1).astype(jnp.int32)
    pos_second = jnp.concatenate([p[1] for p in pos], axis=1).astype(jnp.int32)
    slot_first = jnp.where(pos_first < capacity, first_id * capacity + pos_first, -1)
    slot_second = jnp.where(used & (pos_second < capacity), second_id * capacity + pos_second, -1)

    def build_weights():
        loads[3].wait()
        logits = lax.dot_general(wg[...], tok[...], (((1,), (1,)), ((), ())), preferred_element_type=F32)
        top = jnp.max(logits, axis=0, keepdims=True)
        raised = jnp.exp(logits - top)
        probs = raised / jnp.sum(raised, axis=0, keepdims=True)
        expert_row = lax.broadcasted_iota(jnp.int32, (expert_count, token_count), 0)
        gate_first = jnp.sum(jnp.where(expert_row == first_id, probs, 0.0), axis=0, keepdims=True)
        gate_second = jnp.sum(jnp.where((expert_row == second_id) & used, probs, 0.0), axis=0, keepdims=True)
        gate_total = gate_first + gate_second
        lines = jnp.concatenate(
            [slot_first.astype(F32), slot_second.astype(F32), gate_first / gate_total, gate_second / gate_total,
             jnp.zeros((124, token_count), F32)], axis=0)
        cols[...] = jnp.transpose(lines)
        block = 64
        for c in range(chunks):
            lane = lax.broadcasted_iota(jnp.int32, (1, span), 1)
            slot = lane % rows
            for j in range(CHUNK):
                slot = slot + jnp.where(lane // rows == j, dst[c * CHUNK + j] * rows, 0)
            slot = slot.astype(F32)

            @pl.loop(0, token_count // block)
            def _(i):
                r = pl.ds(pl.multiple_of(i * block, block), block)
                line = cols[r, :]
                weight = jnp.where(line[:, 0:1] == slot, line[:, 2:3], 0.0) + jnp.where(line[:, 1:2] == slot, line[:, 3:4], 0.0)
                weight = weight.astype(BF16)
                cw[r, c * span:(c + 1) * span] = weight
                if c == chunks - 1:
                    last_cw[r, :] = weight[:, span // 2:]

    loads[2].wait()
    for lo, hi in [(0, CHUNK // 2), (CHUNK // 2, CHUNK)] + [(c * CHUNK, (c + 1) * CHUNK) for c in range(1, chunks)]:
        if lo == 2 * CHUNK:
            build_weights()
        for k in range(lo, hi):
            slot = dst[k] * rows + lax.broadcasted_iota(jnp.int32, (rows, token_count), 0)
            hit = (slot == slot_first) | (slot == slot_second)
            onehot[(k - lo) * rows:(k - lo + 1) * rows, :] = jnp.where(hit, 1.0, 0.0).astype(BF16)
        for col in range(0, model_dim, width):
            picked = jnp.dot(onehot[:(hi - lo) * rows, :], tok[:, col:col + width], preferred_element_type=F32).astype(BF16)
            for k in range(lo, hi):
                target = recv if k == self_step else send
                target[k, :, col:col + width] = picked[(k - lo) * rows:(k - lo + 1) * rows]
        if lo == 0:
            pl.semaphore_wait(barrier, len(near))
        if lo == first_far:
            pl.semaphore_wait(ready_sem, len(near))
        for k in range(lo, hi):
            if k != self_step:
                start_forth(k)
        if lo == CHUNK // 2:
            for k in near:
                pl.semaphore_signal(ready_sem, inc=1, device_id={"ep": dst[k]}, device_id_type=MESH)
        if lo == 0:
            for load in loads[4:]:
                load.start()

    for load in loads[4:]:
        load.wait()
    for c in range(chunks):
        wait_forth(c)

        @pl.loop(0, local_experts)
        def _(e):
            r = pl.ds(pl.multiple_of(e * capacity, capacity), capacity)
            x = recv[c * CHUNK:(c + 1) * CHUNK, r, :].reshape(CHUNK * capacity, model_dim)
            y = jnp.zeros((CHUNK * capacity, model_dim), F32)
            tile = 768
            for h in range(0, hidden_dim, tile):
                hidden = jnp.dot(x, wi[e, :, h:h + tile], preferred_element_type=F32)
                hidden = jnp.maximum(hidden, 0.0).astype(BF16)
                y = y + jnp.dot(hidden, wo[e, h:h + tile, :], preferred_element_type=F32)
            y = y.astype(BF16).reshape(CHUNK, capacity, model_dim)
            back[c * CHUNK:(c + 1) * CHUNK, r, :] = y
            if self_step // CHUNK == c:
                home[self_step, r, :] = y[self_step % CHUNK]

        for k in range(c * CHUNK, (c + 1) * CHUNK):
            if k != self_step:
                start_home(k)

    block = 256
    for run, (lo, hi) in enumerate(home_runs[:-1]):
        wait_home(run)

        @pl.loop(0, token_count // block)
        def _(i):
            r = pl.ds(pl.multiple_of(i * block, block), block)
            y = home[lo:hi].reshape((hi - lo) * rows, model_dim)
            part = jnp.dot(cw[r, lo * rows:hi * rows], y, preferred_element_type=F32)
            if lo > 0:
                part = acc[r, :] + part
            acc[r, :] = part

    lo, hi = home_runs[-1]
    wait_home(len(home_runs) - 1)
    last_home[...] = home[lo:hi].reshape((hi - lo) * rows, model_dim)
    for lo, hi in ((0, self_step), (self_step + 1, steps)):
        if lo < hi:
            remote(send, recv, fs_sem, fr_sem, lo, hi, 0, me).wait_send()
            remote(back, home, bs_sem, br_sem, lo, hi, 0, me).wait_send()


def finish_kernel(acc, last_cw, last_home, out_hbm, out, sem):
    block = 256
    copies = []
    for i in range(out.shape[0] // block):
        r = pl.ds(i * block, block)
        part = acc[r, :] + jnp.dot(last_cw[r, :], last_home[...], preferred_element_type=F32)
        out[r, :] = part.astype(BF16)
        copies.append(pltpu.make_async_copy(out.at[r], out_hbm.at[r], sem.at[i]))
        copies[-1].start()
    for copy in copies:
        copy.wait()


def solution(mesh):
    n = mesh.shape["ep"]
    offsets = step_offsets()

    def local_layer(tokens, w_gate, expert_ids, keep_second, w_in, w_out):
        token_count, model_dim = tokens.shape[1:]
        expert_count = w_gate.shape[1]
        local_experts, _, hidden_dim = w_in.shape
        capacity = 2 * token_count // expert_count
        rows = local_experts * capacity
        any_space = pl.BlockSpec(memory_space=pltpu.HBM)
        vmem = pltpu.VMEM
        last = CHUNK // 2 * rows
        parts = pl.pallas_call(
            functools.partial(layer_kernel, n, offsets),
            out_shape=[
                jax.ShapeDtypeStruct((token_count, model_dim), F32),
                jax.ShapeDtypeStruct((token_count, last), BF16),
                jax.ShapeDtypeStruct((last, model_dim), BF16),
            ],
            in_specs=[any_space] * 6,
            out_specs=[pl.BlockSpec(memory_space=vmem)] * 3,
            scratch_shapes=[
                vmem((token_count, model_dim), BF16),
                vmem((expert_count, model_dim), BF16),
                vmem((2, token_count), jnp.int32),
                vmem((1, token_count), jnp.int32),
                vmem(w_in.shape, BF16),
                vmem(w_out.shape, BF16),
                vmem((CHUNK * rows, token_count), BF16),
                vmem((n, rows, model_dim), BF16),
                vmem((n, rows, model_dim), BF16),
                vmem((n, rows, model_dim), BF16),
                vmem((n, rows, model_dim), BF16),
                vmem((token_count, 128), F32),
                vmem((token_count, n * rows), BF16),
                pltpu.SemaphoreType.REGULAR,
                pltpu.SemaphoreType.DMA((6,)),
                pltpu.SemaphoreType.DMA((1,)),
                pltpu.SemaphoreType.DMA((n // CHUNK,)),
                pltpu.SemaphoreType.DMA((1,)),
                pltpu.SemaphoreType.DMA((n // CHUNK + 1,)),
            ],
            compiler_params=pltpu.CompilerParams(
                collective_id=0, has_side_effects=True, vmem_limit_bytes=48 * 1024 * 1024),
            name="moe_layer",
        )(*[pltpu.with_memory_space_constraint(x, pltpu.HBM)
            for x in (tokens[0], w_gate.T, expert_ids[0].T, keep_second, w_in, w_out)])
        out = pl.pallas_call(
            finish_kernel,
            out_shape=jax.ShapeDtypeStruct((token_count, model_dim), BF16),
            in_specs=[pl.BlockSpec(memory_space=vmem)] * 3,
            out_specs=pl.BlockSpec(memory_space=pltpu.HBM),
            scratch_shapes=[vmem((token_count, model_dim), BF16), pltpu.SemaphoreType.DMA((token_count // 256,))],
            compiler_params=pltpu.CompilerParams(vmem_limit_bytes=16 * 1024 * 1024),
            name="finish",
        )(*parts)
        return out[None]

    group_spec = P(("dp", "ep"))
    return jax.shard_map(
        local_layer, mesh=mesh, in_specs=(group_spec, P(), group_spec, group_spec, P("ep"), P("ep")),
        out_specs=group_spec, check_vma=False)
```
